256 devices in a mesh: seq: 64 (over x_hi, z, y), kvh: 4 (over x_lo, core).
Axes of the slice: x: 4 (x_hi: 2, x_lo: 2; x = x_hi * 2 + x_lo), y: 4, z: 8, core: 2. Of those that a mesh axis runs over, the one named last changes fastest.
Arguments:
- queries: bfloat16 [8192, 8192], P('seq', 'kvh'), may hold values from -100 to 100
- keys: bfloat16 [8192, 1024], P('seq', 'kvh'), may hold values from -4 to 4
- values: bfloat16 [8192, 1024], P('seq', 'kvh'), may hold values from -6 to 6
- segments: int32 [8192], P('seq'), may hold values from 0 to 2, never falling along the last dimension, each value on 1 to 4224 neighbouring positions
- basis: bfloat16 [8, 2, 128, 32], P('kvh'), may hold values from -0.5 to 0.5
Outputs:
- attention: bfloat16 [8192, 8192], P('seq', 'kvh')
- latents: bfloat16 [8192, 512], P('seq', 'kvh')
- captured: float32 [8, 2, 32, 32], P('kvh')
- share: float32 [8, 2], P('kvh')
The draws below stay inside these ranges and needn't reach their ends.
Inputs may be any that keep to these rules, and one draw needn't show every extreme that they name: `segments`: document ids never fall along the sequence, and each document has at most 4224 tokens.
All inputs are finite; a program needn't handle non-finite values.
Results may differ from the reference program's by a relative error of at most 0.004.
Values may be sent and summed in bfloat16 or wider, within the bound.
No kernel may reach another device: no remote copies, remote signals or barrier semaphores. Data moves between devices by JAX's collectives and lax.ppermute only.
A program may use at most 64 MiB of HBM per device.

```python
import math
import jax
import jax.numpy as jnp
import numpy as np
from jax import lax

HD = 128
QH = 64
KVH = 8
RANK = 32
TOKENS = 8192
DOC_SPAN = 4224
DOCS = 3


def shared_keys(key):
    normal_part = jax.random.normal(jax.random.fold_in(key, 101), (TOKENS, KVH, HD), jnp.float32)
    column_scale = jnp.exp(jax.random.uniform(jax.random.fold_in(key, 102), (KVH, HD), jnp.float32, jnp.log(0.5), jnp.log(2.0)))
    mixing = jax.random.normal(jax.random.fold_in(key, 103), (KVH, HD, HD), jnp.float32) / jnp.sqrt(float(HD))
    mix_weight = 0.4
    keyed = normal_part * column_scale[None]
    keyed = keyed + mix_weight * jnp.einsum('tgd,gde->tge', keyed, mixing)
    position = jnp.arange(TOKENS, dtype=jnp.float32) / TOKENS
    keyed = keyed * jnp.exp(0.5 * jnp.log(3.0) * position)[:, None, None]
    keyed = jnp.clip(keyed, -4.0, 4.0)
    return keyed


def draw_keys(key, part):
    keyed = shared_keys(key)
    return keyed.reshape(TOKENS, KVH * HD).astype(jnp.bfloat16)


def draw_queries(key, part):
    query_vals = jnp.clip(jax.random.normal(jax.random.fold_in(key, 107), (TOKENS, KVH, QH // KVH, HD), jnp.float32), -4.0, 4.0)
    return query_vals.reshape(TOKENS, QH * HD).astype(jnp.bfloat16)


def levels(own_key, shape, split, low, top_value):
    def one(dim, blocks):
        steps = jax.random.uniform(jax.random.fold_in(jax.random.fold_in(own_key, 6), dim), (blocks,), jnp.float32, low / len(split), top_value / len(split))
        return jnp.repeat(jnp.exp(steps), shape[dim] // blocks).reshape((-1,) + (1,) * (len(shape) - dim - 1))

    level = one(*split[0])
    for cut in split[1:]:
        level = level * one(*cut)
    return level


def profile(count, total, bound, slope):
    portions = [(1 << 20) // math.isqrt(grade ** slope) + 1 for grade in range(2, count + 1)]
    rest, holding = total - bound - (count - 1), [1] * (count - 1)
    while rest > 0:
        candidates = [i for i in range(count - 1) if holding[i] < bound]
        whole, remaining = sum([portions[i] for i in candidates]), rest
        for i in candidates:
            addition = min(bound - holding[i], max(1, remaining * portions[i] // whole), rest)
            holding[i] = holding[i] + addition
            rest = rest - addition
    return np.array([bound] + holding)


def uneven(rng, count, total, most, lean):
    if count == 2:
        one = jax.random.randint(rng, (), max(1, total - most), min(most, total - 1) + 1)
        return jnp.stack([one, total - one])
    tallies = jnp.asarray(profile(count, total, most, lean), jnp.int32)
    couples = (count - 1) // 2
    source_of, receiver = tallies[1:1 + 2 * couples:2], tallies[2:2 + 2 * couples:2]
    margin = jnp.minimum(source_of - 1, most - receiver)
    passed = jax.random.randint(jax.random.fold_in(rng, 1), (couples,), 0, 1 << 20) % (margin + 1)
    tallies = tallies.at[1:1 + 2 * couples:2].set(source_of - passed).at[2:2 + 2 * couples:2].set(receiver + passed)
    return tallies[jax.random.permutation(jax.random.fold_in(rng, 2), count)]


def normal_values(key, shape, spread, bound, split=(), held_as=jnp.bfloat16):
    drawn = jax.random.normal(key, shape, jnp.float32) * spread
    if len(split) > 0:
        drawn = levels(key, shape, split, -0.22, 0.18) * drawn
    return jnp.clip(drawn, min=-bound, max=bound).astype(held_as)


def setup_inputs(seed: int = 0) -> dict:
    splits = jax.random.split(jax.random.key(seed), 6)
    return {
        "queries": draw_queries(jax.random.fold_in(splits[5], 71), 0),
        "keys": draw_keys(jax.random.fold_in(splits[5], 71), 0),
        "values": normal_values(splits[2], (TOKENS, KVH * HD), 1.0, 6.0, ((0, 64), (1, 4))),
        "segments": jnp.searchsorted(jnp.cumsum(uneven(splits[3], DOCS, TOKENS, DOC_SPAN, 1)), jnp.arange(TOKENS), side="right").astype(jnp.int32),
        "basis": normal_values(splits[4], (KVH, 2, HD, RANK), HD ** -0.5, 0.5, ((0, 4),)),
    }


def reference(queries, keys, values, segments, basis):
    per_group = QH // KVH
    q_heads = queries.reshape(TOKENS, KVH, per_group, HD)
    k_heads = keys.reshape(TOKENS, KVH, HD)
    v_heads = values.reshape(TOKENS, KVH, HD)
    q_block = min(512, TOKENS)
    key_span = min(TOKENS, DOC_SPAN + q_block)
    score_scale = float(HD) ** -0.5

    def attend_block(block_number):
        q_start = (block_number * q_block).astype(jnp.int32)
        k_start = jnp.clip(q_start + q_block - key_span, 0, TOKENS - key_span).astype(jnp.int32)
        q_part = lax.dynamic_slice_in_dim(q_heads, q_start, q_block, 0)
        k_part = lax.dynamic_slice_in_dim(k_heads, k_start, key_span, 0)
        v_part = lax.dynamic_slice_in_dim(v_heads, k_start, key_span, 0)
        seg_query = lax.dynamic_slice_in_dim(segments, q_start, q_block, 0)
        seg_keys = lax.dynamic_slice_in_dim(segments, k_start, key_span, 0)
        query_pos = q_start + jnp.arange(q_block, dtype=jnp.int32)
        key_pos = k_start + jnp.arange(key_span, dtype=jnp.int32)
        allowed = (key_pos[None, :] <= query_pos[:, None]) & (seg_keys[None, :] == seg_query[:, None])
        scores = jnp.einsum('tgjd,sgd->gjts', q_part.astype(jnp.float32), k_part.astype(jnp.float32)) * score_scale
        scores = jnp.where(allowed, scores, -1e30)
        row_max = jnp.max(scores, axis=-1, keepdims=True)
        expo = jnp.where(allowed, jnp.exp(scores - row_max), 0.0)
        row_sum = jnp.sum(expo, axis=-1)
        rounded = lax.optimization_barrier(expo.astype(jnp.bfloat16))
        mixed = jnp.einsum('gjts,sgd->tgjd', rounded.astype(jnp.float32), v_part.astype(jnp.float32))
        mixed = mixed / jnp.transpose(row_sum, (2, 0, 1))[..., None]
        return mixed.astype(jnp.bfloat16)

    attention = lax.map(attend_block, jnp.arange(TOKENS // q_block, dtype=jnp.int32)).reshape(TOKENS, QH * HD)
    k_float = k_heads.astype(jnp.float32)
    v_float = v_heads.astype(jnp.float32)
    gram = jnp.stack([jnp.einsum('tgd,tge->gde', k_float, k_float, precision=lax.Precision.HIGHEST),
                      jnp.einsum('tgd,tge->gde', v_float, v_float, precision=lax.Precision.HIGHEST)], axis=1)
    basis_f32 = basis.astype(jnp.float32)
    captured = jnp.einsum('hcdr,hcde,hces->hcrs', basis_f32, gram, basis_f32, precision=lax.Precision.HIGHEST) / TOKENS
    energy = jnp.trace(gram, axis1=2, axis2=3)
    share = KVH * energy / jnp.sum(energy, axis=0, keepdims=True)
    key_lat = jnp.einsum('tgd,gdr->tgr', k_float, basis_f32[:, 0])
    value_lat = jnp.einsum('tgd,gdr->tgr', v_float, basis_f32[:, 1])
    latents = jnp.concatenate([key_lat, value_lat], axis=-1).astype(jnp.bfloat16).reshape(TOKENS, KVH * 2 * RANK)
    return attention, latents, captured, share
```

```python
import functools
import math

import jax
import jax.numpy as jnp
from jax import lax
from jax.experimental import pallas as pl
from jax.experimental.pallas import tpu as pltpu
from jax.sharding import Mesh
from jax.sharding import PartitionSpec as P

HD = 128
QH = 64
KVH = 8
RANK = 32
TOKENS = 8192
SLABS = 16
SEQ = ("a", "z", "y")
KV = ("xl", "c")
RING = ("a", "z")
COLUMN = ("y", "c")
BLOCK = 144
HALF = 2 * BLOCK
SCALE2 = HD**-0.5 * math.log2(math.e)
FIRST = -1e30
MASKED = -2e30
FAR = 1e9

GROUPS = ((0, 1, 8, 2, 7), (3, 6, 4, 5))


def to_heads(t):
    pairs = []
    for y in range(4):
        for c in range(2):
            head = (y & 1) ^ t
            pairs.append((y * 2 + c, (2 * c + head) * 2 + (y >> 1)))
    return pairs


def shifted(array, by):
    return lax.ppermute(array, RING, [(i, (i + by) % SLABS) for i in range(SLABS)])


def added(array, axis, distance):
    size = lax.axis_size(axis)
    return array + lax.ppermute(array, axis, [(i, i ^ distance) for i in range(size)])


def local_kernel(where_ref, keys_ref, values_ref, basis_ref, latents_ref, stats_ref):
    kvh = where_ref[0]
    lane = lax.broadcasted_iota(jnp.int32, (8, 128), 1)
    projected = []
    energies = jnp.zeros((8, 128), jnp.float32)
    for g in range(2):
        for kind, ref in enumerate((keys_ref, values_ref)):
            rows = ref[:, g * HD : (g + 1) * HD]
            projected.append(
                jnp.dot(rows, basis_ref[g, kind], preferred_element_type=jnp.float32)
            )
            squares = rows.astype(jnp.float32)
            total = jnp.sum(squares * squares)
            energies = jnp.where(lane == kvh * 4 + g * 2 + kind, total, energies)
    latents = jnp.concatenate(projected, axis=1)
    latents_ref[...] = latents.astype(jnp.bfloat16)
    seen = lax.dot_general(
        latents,
        latents,
        (((0,), (0,)), ((), ())),
        precision=lax.Precision.HIGHEST,
        preferred_element_type=jnp.float32,
    )
    wide = lax.broadcasted_iota(jnp.int32, (RANK, 128), 1) // RANK
    packed = jnp.zeros((RANK, 128), jnp.float32)
    for n in range(4):
        packed = jnp.where(wide == n, seen[n * RANK : (n + 1) * RANK, :], packed)
    row = lax.broadcasted_iota(jnp.int32, (8, 128), 0)
    stats_ref[0:RANK, :] = packed
    stats_ref[RANK : RANK + 8, :] = jnp.where(row == 0, energies, 0.0)


def attend_kernel(count, tail, first, last, *refs):
    refs = list(refs)
    where_ref, q0_ref, q1_ref, mine_ref, theirs_ref = refs[:5]
    refs = refs[5:]
    if not first:
        starts_in, top_in, sum_in, mix_in = refs[:4]
        refs = refs[4:]
    if last:
        out_refs = refs[:2]
        starts_ref, top_ref, sum_ref, mix_ref = refs[2:]
    else:
        starts_ref, top_ref, sum_ref, mix_ref = refs
    slab, core, odd = where_ref[0], where_ref[1], where_ref[2]

    def pieces(i, with_tail):
        at = where_ref[3 + i] * 512
        found = []
        for ref, half in ((mine_ref, core), (theirs_ref, 1 - core)):
            if with_tail:
                found.append((ref, i * HALF, at + half * 256 + 128))
            else:
                for t in range(2):
                    found.append((ref, i * HALF + t * BLOCK, at + half * 256 + (odd ^ t) * 128))
        return found

    if first:
        one = jnp.full((16, 128), FAR, jnp.float32)
        two = one
    else:
        one = starts_in[0:16, :]
        two = starts_in[16:32, :]
    for i in range(count + int(tail)):
        for ref, row, base in pieces(i, i == count):
            counts = ref[row + 128 : row + BLOCK, :].astype(jnp.float32)
            at = base.astype(jnp.float32)
            n1, n2 = counts[:, :128], counts[:, 128:]
            one = jnp.minimum(one, jnp.where(n1 < 128.0, at + n1, FAR))
            two = jnp.minimum(two, jnp.where(n2 < 128.0, at + n2, FAR))
    starts_ref[0:16, :] = one
    starts_ref[16:32, :] = two
    start1 = jnp.min(one).astype(jnp.int32)
    start2 = jnp.min(two).astype(jnp.int32)

    if first:
        top_ref[...] = jnp.full(top_ref.shape, FIRST, jnp.float32)
        sum_ref[...] = jnp.zeros(sum_ref.shape, jnp.float32)
        mix_ref[...] = jnp.zeros(mix_ref.shape, jnp.float32)
    else:
        top_ref[...] = top_in[...]
        sum_ref[...] = sum_in[...]
        mix_ref[...] = mix_in[...]

    q_base = [slab * 512 + core * 256 + (odd ^ t) * 128 for t in range(2)]
    row_iota = lax.broadcasted_iota(jnp.int32, (128, 128), 0)
    lane_iota = lax.broadcasted_iota(jnp.int32, (128, 128), 1)

    def slab_step(i, with_tail):
        found = pieces(i, with_tail)
        at = where_ref[3 + i] * 512
        for t, q_ref in enumerate((q0_ref, q1_ref)):
            low = jnp.where(
                q_base[t] >= start2, start2, jnp.where(q_base[t] >= start1, start1, 0)
            )
            needed = (at <= q_base[t] + 127) & (at + 511 >= low)

            @pl.when(needed)
            def _(t=t, q_ref=q_ref):
                q_pos = q_base[t] + row_iota
                lows = jnp.where(
                    q_pos >= start2, start2, jnp.where(q_pos >= start1, start1, 0)
                )
                allowed, k_parts, v_parts = [], [], []
                for ref, row, base in found:
                    k_pos = base + lane_iota
                    allowed.append((k_pos >= lows) & (k_pos <= q_pos))
                    rows = pl.ds(row, 128) if isinstance(row, int) else pl.ds(pl.multiple_of(row, 16), 128)
                    k_parts.append(ref[rows, 0:HD])
                    v_parts.append(ref[rows, HD : 2 * HD])
                k = jnp.concatenate(k_parts, axis=0)
                v = jnp.concatenate(v_parts, axis=0)
                for pair in range(4):
                    heads = (2 * pair, 2 * pair + 1)
                    q = jnp.concatenate([q_ref[:, j * HD : (j + 1) * HD] for j in heads], axis=0)
                    scores = lax.dot_general(
                        q, k, (((1,), (1,)), ((), ())), preferred_element_type=jnp.float32
                    )
                    parts = []
                    for n, mask in enumerate(allowed):
                        mask2 = jnp.concatenate([mask, mask], axis=0)
                        parts.append(
                            jnp.where(mask2, scores[:, n * 128 : (n + 1) * 128], MASKED)
                        )
                    best = functools.reduce(jnp.maximum, parts)
                    span = slice(t * 1024 + pair * 256, t * 1024 + pair * 256 + 256)
                    top_old = top_ref[span, :]
                    top = jnp.maximum(top_old, jnp.max(best, axis=1, keepdims=True))
                    factor = jnp.exp2((top_old - top) * SCALE2)
                    weights = [jnp.exp2((part - top) * SCALE2) for part in parts]
                    sum_ref[span, :] = sum_ref[span, :] * factor + functools.reduce(
                        jnp.add, weights
                    )
                    rounded = jnp.concatenate([w.astype(jnp.bfloat16) for w in weights], axis=1)
                    mix_ref[span, :] = mix_ref[span, :] * factor + jnp.dot(
                        rounded, v, preferred_element_type=jnp.float32
                    )
                    top_ref[span, :] = top

    def loop_step(i, carry):
        slab_step(i, False)
        return carry

    lax.fori_loop(0, count, loop_step, 0)
    if tail:
        slab_step(count, True)
    if last:
        for t in range(2):
            for j in range(8):
                span = slice(t * 1024 + j * 128, t * 1024 + (j + 1) * 128)
                total = jnp.sum(sum_ref[span, :], axis=1, keepdims=True)
                out_refs[t][:, j * HD : (j + 1) * HD] = (mix_ref[span, :] / total).astype(
                    jnp.bfloat16
                )


def vmem():
    return pl.BlockSpec(memory_space=pltpu.VMEM)


def attend(where, q0, q1, mine, theirs, state, count, tail, last):
    first = state is None
    carry = [
        jax.ShapeDtypeStruct((32, 128), jnp.float32),
        jax.ShapeDtypeStruct((2048, 128), jnp.float32),
        jax.ShapeDtypeStruct((2048, 128), jnp.float32),
        jax.ShapeDtypeStruct((2048, 128), jnp.float32),
    ]
    keys = count * 512 + (256 if tail else 0)
    cost = pl.CostEstimate(
        flops=4 * 2048 * keys * HD, bytes_accessed=4 * 1024 * 1024, transcendentals=2048 * keys
    )
    if last:
        out_shape = [jax.ShapeDtypeStruct((128, 1024), jnp.bfloat16)] * 2
        scratch = [pltpu.VMEM(c.shape, c.dtype) for c in carry]
    else:
        out_shape, scratch = carry, []
    inputs = [q0, q1, mine, theirs] + ([] if first else list(state))
    return pl.pallas_call(
        functools.partial(attend_kernel, count, tail, first, last),
        out_shape=out_shape,
        in_specs=[pl.BlockSpec(memory_space=pltpu.SMEM)] + [vmem()] * len(inputs),
        out_specs=[vmem()] * len(out_shape),
        scratch_shapes=scratch,
        compiler_params=pltpu.CompilerParams(vmem_limit_bytes=24 * 1024 * 1024),
        cost_estimate=cost,
        name="attend_last" if last else "attend",
    )(where, *inputs)


def body(queries, keys, values, segments, basis):
    a, z, y = lax.axis_index("a"), lax.axis_index("z"), lax.axis_index("y")
    c, xl = lax.axis_index("c"), lax.axis_index("xl")
    odd = y & 1
    kvh = xl * 2 + c
    slab = a * 8 + z

    n1 = jnp.sum((segments < 1).astype(jnp.float32))
    n2 = jnp.sum((segments < 2).astype(jnp.float32))
    lanes = lax.broadcasted_iota(jnp.int32, (16, 256), 1)
    counts = jnp.where(lanes < 128, n1, n2).astype(jnp.bfloat16)

    def block_of(head):
        return jnp.concatenate(
            [
                jnp.concatenate(
                    [
                        lax.dynamic_slice_in_dim(keys, head * HD, HD, 1),
                        lax.dynamic_slice_in_dim(values, head * HD, HD, 1),
                    ],
                    axis=1,
                ),
                counts,
            ],
            axis=0,
        )

    kv = [lax.ppermute(block_of(odd ^ t), COLUMN, to_heads(t)) for t in range(2)]
    q = [
        lax.ppermute(
            lax.dynamic_slice_in_dim(queries, (odd ^ t) * 1024, 1024, 1), COLUMN, to_heads(t)
        )
        for t in range(2)
    ]

    at = {0: jnp.concatenate(kv, axis=0)}
    at[1] = shifted(at[0], 1)
    at[8] = shifted(at[0], 8)
    at[2] = shifted(at[1], 1)
    at[7] = shifted(at[8], -1)
    tail = shifted(jnp.where(odd == 0, at[8][BLOCK:], at[8][:BLOCK]), 1)
    at[3] = shifted(at[2], 1)
    at[6] = shifted(at[7], -1)
    at[4] = shifted(at[3], 1)
    at[5] = shifted(at[6], -1)

    latents, stats = pl.pallas_call(
        local_kernel,
        out_shape=[
            jax.ShapeDtypeStruct((128, 128), jnp.bfloat16),
            jax.ShapeDtypeStruct((RANK + 8, 128), jnp.float32),
        ],
        in_specs=[pl.BlockSpec(memory_space=pltpu.SMEM)] + [vmem()] * 3,
        out_specs=[vmem()] * 2,
        cost_estimate=pl.CostEstimate(
            flops=1 << 26, bytes_accessed=1 << 18, transcendentals=0
        ),
        name="local",
    )(kvh.reshape(1), keys, values, basis)

    state = None
    for n, group in enumerate(GROUPS):
        last = n == len(GROUPS) - 1
        mine = [at[d] for d in group] + ([tail] if last else [])
        mine = jnp.concatenate(mine, axis=0)
        theirs = lax.ppermute(mine, "c", [(0, 1), (1, 0)])
        distances = list(group) + ([9] if last else [])
        where = jnp.stack([slab, c, odd] + [(slab - d) % SLABS for d in distances])
        where = where.astype(jnp.int32)
        state = attend(where, q[0], q[1], mine, theirs, state, len(group), last, last)

    back = [
        lax.ppermute(state[t], COLUMN, [(d, s) for s, d in to_heads(t)]) for t in range(2)
    ]
    attention = jnp.where(
        odd == 0, jnp.concatenate(back, axis=1), jnp.concatenate(back[::-1], axis=1)
    )

    for axis, distance in (("y", 1), ("y", 2), ("z", 1), ("z", 2), ("z", 4), ("a", 1)):
        stats = added(stats, axis, distance)
    seen = stats[:RANK].reshape(RANK, 4, RANK).transpose(1, 0, 2).reshape(2, 2, RANK, RANK)
    captured = seen / TOKENS
    energies = added(added(stats[RANK:], "c", 1), "xl", 1)[0, : 2 * KVH].reshape(KVH, 2)
    own = lax.dynamic_slice_in_dim(energies, kvh * 2, 2, 0)
    share = KVH * own / jnp.sum(energies, axis=0)[None, :]
    return (attention, latents, captured, share)


def solution(mesh):
    torus = Mesh(mesh.devices.reshape(2, 8, 4, 2, 2), ("a", "z", "y", "xl", "c"))
    in_specs = (P(SEQ, KV), P(SEQ, KV), P(SEQ, KV), P(SEQ), P(KV, None, None, None))
    out_specs = (P(SEQ, KV), P(SEQ, KV), P(KV, None, None, None), P(KV, None))
    return jax.shard_map(body, mesh=torus, in_specs=in_specs, out_specs=out_specs, check_vma=False)
```

```python
import functools
import math

import jax
import jax.numpy as jnp
from jax import lax
from jax.experimental import pallas as pl
from jax.experimental.pallas import tpu as pltpu
from jax.sharding import Mesh
from jax.sharding import PartitionSpec as P

HD = 128
QH = 64
KVH = 8
RANK = 32
TOKENS = 8192
SLABS = 16
SEQ = ("a", "z", "y")
KV = ("xl", "c")
RING = ("a", "z")
COLUMN = ("y", "c")
BLOCK = 144
HALF = 2 * BLOCK
SCALE2 = HD**-0.5 * math.log2(math.e)
FIRST = -1e30
MASKED = -2e30
FAR = 1e9


def to_heads(t):
    pairs = []
    for y in range(4):
        for c in range(2):
            head = (y & 1) ^ t
            pairs.append((y * 2 + c, (2 * c + head) * 2 + (y >> 1)))
    return pairs


def shifted(array, by):
    return lax.ppermute(array, RING, [(i, (i + by) % SLABS) for i in range(SLABS)])


def partners(array, first_axis, first, second_axis, second):
    axes = (first_axis,) if first_axis == second_axis else (first_axis, second_axis)
    sizes = [lax.axis_size(axis) for axis in axes]
    width = sizes[-1]
    one = first if len(axes) == 1 else first * width
    total = math.prod(sizes)
    return [
        lax.ppermute(array, axes, [(i, i ^ change) for i in range(total)])
        for change in (one, second, one ^ second)
    ]


def local_kernel(where_ref, keys_ref, values_ref, basis_ref, after_ref, latents_ref, stats_ref):
    kvh = where_ref[0]
    lane = lax.broadcasted_iota(jnp.int32, (8, 128), 1)
    projected = []
    energies = jnp.zeros((8, 128), jnp.float32)
    for g in range(2):
        for kind, ref in enumerate((keys_ref, values_ref)):
            rows = ref[:, g * HD : (g + 1) * HD]
            projected.append(
                jnp.dot(rows, basis_ref[g, kind], preferred_element_type=jnp.float32)
            )
            squares = rows.astype(jnp.float32)
            total = jnp.sum(squares * squares)
            energies = jnp.where(lane == kvh * 4 + g * 2 + kind, total, energies)
    latents = jnp.concatenate(projected, axis=1)
    latents_ref[...] = latents.astype(jnp.bfloat16)
    seen = lax.dot_general(
        latents,
        latents,
        (((0,), (0,)), ((), ())),
        precision=lax.Precision.HIGHEST,
        preferred_element_type=jnp.float32,
    )
    wide = lax.broadcasted_iota(jnp.int32, (RANK, 128), 1) // RANK
    packed = jnp.zeros((RANK, 128), jnp.float32)
    for n in range(4):
        packed = jnp.where(wide == n, seen[n * RANK : (n + 1) * RANK, :], packed)
    row = lax.broadcasted_iota(jnp.int32, (8, 128), 0)
    stats_ref[0:RANK, :] = packed
    stats_ref[RANK : RANK + 8, :] = jnp.where(row == 0, energies, 0.0)


def prepare_kernel(where_ref, keys_ref, values_ref, segments_ref, first_ref, second_ref):
    ids = segments_ref[...]
    n1 = jnp.sum((ids < 1).astype(jnp.float32))
    n2 = jnp.sum((ids < 2).astype(jnp.float32))
    lanes = lax.broadcasted_iota(jnp.int32, (16, 256), 1)
    counts = jnp.where(lanes < 128, n1, n2).astype(jnp.bfloat16)
    for odd in range(2):

        @pl.when(where_ref[0] == odd)
        def _(odd=odd):
            for ref, head in ((first_ref, odd), (second_ref, 1 - odd)):
                ref[0:128, 0:HD] = keys_ref[:, head * HD : (head + 1) * HD]
                ref[0:128, HD : 2 * HD] = values_ref[:, head * HD : (head + 1) * HD]

    for ref in (first_ref, second_ref):
        ref[128:BLOCK, :] = counts


def attend_kernel(halves, tiles, first, last, adds, *refs):
    refs = list(refs)
    where_ref = refs.pop(0)
    if first:
        q_in = [refs.pop(0) for _ in range(2)]
    key_refs = [refs.pop(0) for _ in halves]
    state_in = None if first else [refs.pop(0) for _ in range(5)]
    if adds:
        terms = [refs.pop(0) for _ in range(4)]
        added_ref = refs.pop(1 if last else 5)
        added_ref[...] = (terms[0][...] + terms[1][...]) + (terms[2][...] + terms[3][...])
    if last:
        out_ref = refs.pop(0)
        q_ref, starts_ref = state_in[0], state_in[1]
        top_ref, sum_ref, mix_ref = refs
    else:
        q_ref, starts_ref, top_ref, sum_ref, mix_ref = refs
    slab, core, odd = where_ref[0], where_ref[1], where_ref[2]
    origin = tiles[0] * 1024 if last else 0

    units = []
    for ref, parts in zip(key_refs, halves):
        row, found = 0, []
        for index, theirs, rounds in parts:
            base = where_ref[3 + index] * 512 + (1 - core if theirs else core) * 256
            for t in rounds:
                block = base + (128 if t is None else (odd ^ t) * 128)
                found.append((ref, row, block))
                row += BLOCK
        units.append(found)

    one = jnp.full((16, 128), FAR, jnp.float32) if first else state_in[1][0:16, :]
    two = jnp.full((16, 128), FAR, jnp.float32) if first else state_in[1][16:32, :]
    for found in units:
        for ref, row, base in found:
            counts = ref[row + 128 : row + BLOCK, :].astype(jnp.float32)
            at = base.astype(jnp.float32)
            n1, n2 = counts[:, :128], counts[:, 128:]
            one = jnp.minimum(one, jnp.where(n1 < 128.0, at + n1, FAR))
            two = jnp.minimum(two, jnp.where(n2 < 128.0, at + n2, FAR))
    if not last:
        starts_ref[0:16, :] = one
        starts_ref[16:32, :] = two
    start1 = jnp.min(one).astype(jnp.int32)
    start2 = jnp.min(two).astype(jnp.int32)

    if first:
        for t in range(2):
            for j in range(8):
                q_ref[t * 1024 + j * 128 : t * 1024 + (j + 1) * 128, :] = q_in[t][
                    :, j * HD : (j + 1) * HD
                ]
        top_ref[...] = jnp.full(top_ref.shape, FIRST, jnp.float32)
        sum_ref[...] = jnp.zeros(sum_ref.shape, jnp.float32)
        mix_ref[...] = jnp.zeros(mix_ref.shape, jnp.float32)
    elif last:
        span = slice(origin, origin + 1024)
        top_ref[...] = state_in[2][span, :]
        sum_ref[...] = state_in[3][span, :]
        mix_ref[...] = state_in[4][span, :]

    row_iota = lax.broadcasted_iota(jnp.int32, (128, 128), 0)
    lane_iota = lax.broadcasted_iota(jnp.int32, (128, 128), 1)

    def tile_step(t):
        q_base = slab * 512 + core * 256 + (odd ^ t) * 128

        def low_of(position):
            return jnp.where(
                position >= start2, start2, jnp.where(position >= start1, start1, 0)
            )

        low = low_of(q_base)
        for found in units:
            needed = functools.reduce(
                jnp.logical_or,
                [(base <= q_base) & (base + 127 >= low) for ref, row, base in found],
            )

            @pl.when(needed)
            def _(found=found):
                q_pos = q_base + row_iota
                lows = low_of(q_pos)
                allowed = []
                for ref, row, base in found:
                    k_pos = base + lane_iota
                    allowed.append((k_pos >= lows) & (k_pos <= q_pos))
                k = jnp.concatenate([r[row : row + 128, 0:HD] for r, row, _ in found], axis=0)
                v = jnp.concatenate([r[row : row + 128, HD:] for r, row, _ in found], axis=0)
                for pair in range(4):
                    at = t * 1024 + pair * 256
                    q = q_ref[pl.ds(at, 256), :]
                    scores = lax.dot_general(
                        q, k, (((1,), (1,)), ((), ())), preferred_element_type=jnp.float32
                    )
                    parts = []
                    for n, mask in enumerate(allowed):
                        mask2 = jnp.concatenate([mask, mask], axis=0)
                        parts.append(
                            jnp.where(mask2, scores[:, n * 128 : (n + 1) * 128], MASKED)
                        )
                    best = functools.reduce(jnp.maximum, parts)
                    span = pl.ds(at - origin, 256)
                    top_old = top_ref[span, :]
                    top = jnp.maximum(top_old, jnp.max(best, axis=1, keepdims=True))
                    factor = jnp.exp2((top_old - top) * SCALE2)
                    weights = [jnp.exp2((part - top) * SCALE2) for part in parts]
                    sum_ref[span, :] = sum_ref[span, :] * factor + functools.reduce(
                        jnp.add, weights
                    )
                    rounded = jnp.concatenate([w.astype(jnp.bfloat16) for w in weights], axis=1)
                    mix_ref[span, :] = mix_ref[span, :] * factor + jnp.dot(
                        rounded, v, preferred_element_type=jnp.float32
                    )
                    top_ref[span, :] = top

    if len(tiles) == 1:
        tile_step(tiles[0])
    else:

        def loop_step(t, carry):
            tile_step(t)
            return carry

        lax.fori_loop(0, 2, loop_step, 0)
    if last:
        for j in range(8):
            span = slice(j * 128, (j + 1) * 128)
            total = jnp.sum(sum_ref[span, :], axis=1, keepdims=True)
            out_ref[:, j * HD : (j + 1) * HD] = (mix_ref[span, :] / total).astype(jnp.bfloat16)


def finish_kernel(where_ref, stats_ref, one_ref, two_ref, three_ref, captured_ref, share_ref):
    kvh = where_ref[0]
    for n in range(4):
        captured_ref[n] = stats_ref[0:RANK, n * RANK : (n + 1) * RANK] * (1.0 / TOKENS)
    energies = stats_ref[RANK : RANK + 8, :] + one_ref[...] + two_ref[...] + three_ref[...]
    lane = lax.broadcasted_iota(jnp.int32, (8, 128), 1)
    rows = lax.broadcasted_iota(jnp.int32, (2, 2), 0)
    columns = lax.broadcasted_iota(jnp.int32, (2, 2), 1)
    share = jnp.zeros((2, 2), jnp.float32)
    for kind in range(2):
        total = jnp.sum(jnp.where(lane % 2 == kind, energies, 0.0))
        for g in range(2):
            own = jnp.sum(jnp.where(lane == kvh * 4 + g * 2 + kind, energies, 0.0))
            value = jnp.full((2, 2), KVH * own, jnp.float32) / total
            share = jnp.where((rows == g) & (columns == kind), value, share)
    share_ref[...] = share


def vmem():
    return pl.BlockSpec(memory_space=pltpu.VMEM)


def small():
    return pltpu.CompilerParams(vmem_limit_bytes=4 * 1024 * 1024)


def attend(where, q, arrays, halves, state, tile=None, terms=()):
    first, last = state is None, tile is not None
    wide = (2048, 128)
    carry = [
        jax.ShapeDtypeStruct(wide, jnp.bfloat16),
        jax.ShapeDtypeStruct((32, 128), jnp.float32),
        jax.ShapeDtypeStruct(wide, jnp.float32),
        jax.ShapeDtypeStruct(wide, jnp.float32),
        jax.ShapeDtypeStruct(wide, jnp.float32),
    ]
    tiles = (tile,) if last else (0, 1)
    work = len(tiles) * 1024 * sum(a.shape[0] for a in arrays)
    inputs = (list(q) if first else []) + list(arrays)
    aliases = {}
    if not first:
        if not last:
            aliases = {1 + len(inputs) + n: n for n in range(5)}
        inputs += list(state)
    inputs += list(terms)
    if last:
        out_shape = [jax.ShapeDtypeStruct((128, 1024), jnp.bfloat16)]
        scratch = [pltpu.VMEM((1024, 128), jnp.float32)] * 3
    else:
        out_shape, scratch = carry, []
    if terms:
        out_shape = out_shape + [jax.ShapeDtypeStruct(terms[0].shape, jnp.float32)]
    out_specs = [vmem()] * len(out_shape)
    return pl.pallas_call(
        functools.partial(attend_kernel, halves, tiles, first, last, bool(terms)),
        out_shape=out_shape,
        in_specs=[pl.BlockSpec(memory_space=pltpu.SMEM)] + [vmem()] * len(inputs),
        out_specs=out_specs,
        scratch_shapes=scratch,
        input_output_aliases=aliases,
        compiler_params=pltpu.CompilerParams(vmem_limit_bytes=16 * 1024 * 1024),
        cost_estimate=pl.CostEstimate(
            flops=4 * work * HD, bytes_accessed=1 << 20, transcendentals=work
        ),
        name="attend_last" if last else "attend",
    )(where, *inputs)


def body(queries, keys, values, segments, basis):
    a, z, y = lax.axis_index("a"), lax.axis_index("z"), lax.axis_index("y")
    c, xl = lax.axis_index("c"), lax.axis_index("xl")
    odd = y & 1
    kvh = xl * 2 + c
    slab = a * 8 + z

    blocks = pl.pallas_call(
        prepare_kernel,
        out_shape=[jax.ShapeDtypeStruct((BLOCK, 256), jnp.bfloat16)] * 2,
        in_specs=[pl.BlockSpec(memory_space=pltpu.SMEM)] + [vmem()] * 3,
        out_specs=[vmem()] * 2,
        compiler_params=small(),
        name="prepare",
    )(odd.reshape(1).astype(jnp.int32), keys, values, segments.reshape(1, 128))
    kv = [lax.ppermute(blocks[t], COLUMN, to_heads(t)) for t in range(2)]
    slices = [lax.dynamic_slice_in_dim(queries, (odd ^ t) * 1024, 1024, 1) for t in range(2)]
    q = [lax.ppermute(slices[t], COLUMN, to_heads(t)) for t in range(2)]
    *kv, _, _ = lax.optimization_barrier((*kv, *slices))

    at = {0: jnp.concatenate(kv, axis=0)}
    at[1] = shifted(at[0], 1)
    at[8] = shifted(at[0], 8)
    at[2] = shifted(at[0], 2)
    at[7] = shifted(at[0], 7)
    at[6] = shifted(at[0], 6)
    at[9] = shifted(jnp.where(odd == 0, kv[1], kv[0]), 9)
    mine, theirs = {}, {}

    def exchange(*group):
        mine[group] = jnp.concatenate([at[d] for d in group], axis=0)
        theirs[group] = lax.ppermute(mine[group], "c", [(0, 1), (1, 0)])

    def received(state, *group):
        state[2], *arrays = lax.optimization_barrier((state[2], *[at[d] for d in group]))
        at.update(zip(group, arrays))

    exchange(0)

    latents, stats = pl.pallas_call(
        local_kernel,
        out_shape=[
            jax.ShapeDtypeStruct((128, 128), jnp.bfloat16),
            jax.ShapeDtypeStruct((RANK + 8, 128), jnp.float32),
        ],
        in_specs=[pl.BlockSpec(memory_space=pltpu.SMEM)]
        + [vmem()] * 3
        + [vmem()],
        out_specs=[vmem()] * 2,
        compiler_params=small(),
        cost_estimate=pl.CostEstimate(flops=1 << 26, bytes_accessed=1 << 18, transcendentals=0),
        name="local",
    )(kvh.reshape(1), keys, values, basis, theirs[(0,)])

    where = jnp.stack([slab, c, odd] + [(slab - d) % SLABS for d in range(10)]).astype(jnp.int32)

    def half(d, partner):
        return (d, partner, (None,) if d == 9 else (0, 1))

    def own(*group):
        return mine[group], tuple(half(d, False) for d in group)

    def other(*group):
        return theirs[group], tuple(half(d, True) for d in group)

    terms = [stats] + partners(stats, "y", 1, "y", 2)

    def step(state, *groups, terms=()):
        arrays = [array for array, _ in groups]
        return list(attend(where, q, arrays, tuple(h for _, h in groups), state, terms=terms))

    state = step(None, own(0), other(0))
    received(state, 1, 8)
    exchange(1, 8)
    *state, stats = step(state, own(1, 8), terms=tuple(terms))
    received(state, 2, 7, 6, 9)
    at[3] = shifted(at[2], 1)
    at[5] = shifted(at[6], -1)
    exchange(2, 7)
    exchange(6, 9)
    terms = [stats] + partners(stats, "z", 1, "z", 2)
    state = step(state, other(1, 8), own(2, 7))
    received(state, 3, 5)
    at[4] = shifted(at[3], 1)
    exchange(3, 5)
    *state, stats = step(state, other(2, 7), own(6, 9), terms=tuple(terms))
    terms = [stats] + partners(stats, "a", 1, "z", 4)
    state = step(state, other(6, 9), own(3, 5))
    received(state, 4)
    exchange(4)
    state = step(state, other(3, 5), own(4))
    array, halves = other(4)
    out0, stats = attend(where, None, [array], (halves,), state, tile=0, terms=tuple(terms))
    energies = partners(stats[RANK:], "xl", 1, "c", 1)
    (out1,) = attend(where, None, [array], (halves,), state, tile=1)
    mixed = [out0, out1]
    back = [lax.ppermute(mixed[t], COLUMN, [(d, s) for s, d in to_heads(t)]) for t in range(2)]
    attention = jnp.where(
        odd == 0, jnp.concatenate(back, axis=1), jnp.concatenate(back[::-1], axis=1)
    )

    captured, share = pl.pallas_call(
        finish_kernel,
        out_shape=[
            jax.ShapeDtypeStruct((4, RANK, RANK), jnp.float32),
            jax.ShapeDtypeStruct((2, 2), jnp.float32),
        ],
        in_specs=[pl.BlockSpec(memory_space=pltpu.SMEM)] + [vmem()] * 4,
        out_specs=[vmem()] * 2,
        compiler_params=small(),
        name="finish",
    )(kvh.reshape(1), stats, *energies)
    captured = captured.reshape(2, 2, RANK, RANK)
    return (attention, latents, captured, share)


def solution(mesh):
    torus = Mesh(mesh.devices.reshape(2, 8, 4, 2, 2), ("a", "z", "y", "xl", "c"))
    in_specs = (P(SEQ, KV), P(SEQ, KV), P(SEQ, KV), P(SEQ), P(KV, None, None, None))
    out_specs = (P(SEQ, KV), P(SEQ, KV), P(KV, None, None, None), P(KV, None))
    return jax.shard_map(body, mesh=torus, in_specs=in_specs, out_specs=out_specs, check_vma=False)
```

```python
import functools
import math

import jax
import jax.numpy as jnp
from jax import lax
from jax.experimental import pallas as pl
from jax.experimental.pallas import tpu as pltpu
from jax.sharding import Mesh
from jax.sharding import PartitionSpec as P

HD = 128
QH = 64
KVH = 8
RANK = 32
TOKENS = 8192
SLABS = 16
SEQ = ("a", "z", "y")
KV = ("xl", "c")
RING = ("a", "z")
COLUMN = ("y", "c")
BLOCK = 144
HALF = 2 * BLOCK
RIDER = 32
SCALE2 = HD**-0.5 * math.log2(math.e)
FIRST = -1e30
MASKED = -2e30
FAR = 1e9


def to_heads(t):
    pairs = []
    for y in range(4):
        for c in range(2):
            head = (y & 1) ^ t
            pairs.append((y * 2 + c, (2 * c + head) * 2 + (y >> 1)))
    return pairs


def shifted(array, by):
    return lax.ppermute(array, RING, [(i, (i + by) % SLABS) for i in range(SLABS)])


def added(array, axis, distance):
    size = lax.axis_size(axis)
    return array + lax.ppermute(array, axis, [(i, i ^ distance) for i in range(size)])


def encoded(total):
    high = total.astype(jnp.bfloat16)
    rest = (total - high.astype(jnp.float32)).astype(jnp.bfloat16)
    return high, rest


def put(ref, row, total):
    ref[row : row + RIDER, 0:128], ref[row : row + RIDER, 128:256] = encoded(total)


def got(ref, row):
    rows = slice(row, row + RIDER)
    return ref[rows, 0:128].astype(jnp.float32) + ref[rows, 128:256].astype(jnp.float32)


def put_wide(ref, total):
    for n, part in enumerate(encoded(total)):
        for m in range(2):
            lanes = slice(m * 256 + n * 128, m * 256 + n * 128 + 128)
            ref[128:BLOCK, lanes] = part[m * 16 : (m + 1) * 16, :]


def got_wide(ref):
    rows = []
    for m in range(2):
        high = ref[128:BLOCK, m * 256 : m * 256 + 128].astype(jnp.float32)
        rest = ref[128:BLOCK, m * 256 + 128 : m * 256 + 256].astype(jnp.float32)
        rows.append(high + rest)
    return jnp.concatenate(rows, axis=0)


def prepare_kernel(
    where_ref,
    queries_hbm,
    keys_hbm,
    values_hbm,
    segments_hbm,
    basis_hbm,
    first_ref,
    second_ref,
    latents_ref,
    energy_ref,
    keys_ref,
    values_ref,
    segments_ref,
    basis_ref,
    semaphores,
):
    loads = [
        pltpu.make_async_copy(source, target, semaphores.at[n])
        for n, (source, target) in enumerate(
            (
                (segments_hbm, segments_ref),
                (keys_hbm, keys_ref),
                (values_hbm, values_ref),
                (basis_hbm, basis_ref),
            )
        )
    ]
    for copy in loads:
        copy.start()
    for t, ref in enumerate((first_ref, second_ref)):
        column = pl.multiple_of((where_ref[0] ^ t) * 1024, 1024)
        copy = pltpu.make_async_copy(
            queries_hbm.at[:, pl.ds(column, 1024)],
            ref.at[0:128, 0:1024],
            semaphores.at[4 + t],
        )
        copy.start()
        loads.append(copy)
    for copy in loads[:4]:
        copy.wait()
    ids = segments_ref[...]
    n1 = jnp.sum((ids < 1).astype(jnp.float32))
    n2 = jnp.sum((ids < 2).astype(jnp.float32))
    lanes = lax.broadcasted_iota(jnp.int32, (16, 256), 1)
    counts = jnp.where(lanes < 128, n1, n2).astype(jnp.bfloat16)
    projected, energies = [], []
    for g in range(2):
        for kind, ref in enumerate((keys_ref, values_ref)):
            rows = ref[:, g * HD : (g + 1) * HD]
            projected.append(
                lax.dot_general(
                    rows,
                    basis_ref[g, kind],
                    (((1,), (1,)), ((), ())),
                    preferred_element_type=jnp.float32,
                )
            )
            squares = rows.astype(jnp.float32)
            energies.append(jnp.sum(squares * squares))
    latents = jnp.concatenate(projected, axis=1)
    latents_ref[...] = latents.astype(jnp.bfloat16)
    seen = lax.dot_general(
        latents,
        latents,
        (((0,), (0,)), ((), ())),
        precision=lax.Precision.HIGHEST,
        preferred_element_type=jnp.float32,
    )
    lane = lax.broadcasted_iota(jnp.int32, (RIDER, 128), 1) // RANK
    row = lax.broadcasted_iota(jnp.int32, (RIDER, 128), 0)
    riders = []
    for g in range(2):
        other = jnp.where(row == 0, energies[2 * g], jnp.where(row == 1, energies[2 * g + 1], 0.0))
        for n in (2 * g, 2 * g + 1):
            other = jnp.where(lane == n, seen[n * RANK : (n + 1) * RANK, :], other)
        riders.append(other)
    row8 = lax.broadcasted_iota(jnp.int32, (8, 128), 0)
    energy_ref[...] = jnp.where(
        row8 == 0,
        energies[0] + energies[2],
        jnp.where(row8 == 1, energies[1] + energies[3], 0.0),
    )
    for odd in range(2):

        @pl.when(where_ref[0] == odd)
        def _(odd=odd):
            for ref, head in ((first_ref, odd), (second_ref, 1 - odd)):
                ref[0:128, 1024 : 1024 + HD] = keys_ref[:, head * HD : (head + 1) * HD]
                ref[0:128, 1024 + HD : 1280] = values_ref[:, head * HD : (head + 1) * HD]
                put_wide(ref, riders[head])

    for ref in (first_ref, second_ref):
        ref[128:BLOCK, 512:1024] = jnp.zeros((16, 512), jnp.bfloat16)
        ref[128:BLOCK, 1024:1280] = counts
    for copy in loads[4:]:
        copy.wait()


def start_kernel(where_ref, first_ref, second_ref, energy_ref, out_ref):
    out_ref[0:BLOCK, :] = first_ref[:, 1024:1280]
    out_ref[BLOCK:HALF, :] = second_ref[:, 1024:1280]
    lane = lax.broadcasted_iota(jnp.int32, (RIDER, 128), 1) // 64
    row = lax.broadcasted_iota(jnp.int32, (RIDER, 128), 0)
    energy = jnp.where(
        row == 2, energy_ref[0:1, :], jnp.where(row == 3, energy_ref[1:2, :], 0.0)
    )
    energy = jnp.where(lane == 1 - where_ref[2], energy, 0.0)
    put(out_ref, HALF, got_wide(first_ref) + got_wide(second_ref) + energy)


def once_kernel(own_ref, eight_ref, up_ref, down_ref):
    both = got(own_ref, HALF) + got(eight_ref, HALF)
    up_ref[0:HALF, :] = own_ref[0:HALF, :]
    down_ref[0:HALF, :] = eight_ref[0:HALF, :]
    put(up_ref, HALF, both)
    put(down_ref, HALF, both)


def twice_kernel(up_ref, one_ref, down_ref, seven_ref, far_up_ref, far_down_ref):
    far_up_ref[0:HALF, :] = up_ref[0:HALF, :]
    far_up_ref[HALF : 2 * HALF, :] = one_ref[0:HALF, :]
    far_up_ref[2 * HALF : 2 * HALF + RIDER, :] = up_ref[HALF : HALF + RIDER, :]
    far_up_ref[2 * HALF + RIDER : 2 * HALF + 2 * RIDER, :] = one_ref[HALF : HALF + RIDER, :]
    far_down_ref[0:HALF, :] = down_ref[0:HALF, :]
    far_down_ref[HALF : 2 * HALF, :] = seven_ref[0:HALF, :]
    put(far_down_ref, 2 * HALF, got(down_ref, HALF) + got(seven_ref, HALF))


def tail_kernel(where_ref, two_three_ref, eight_ref, out_ref):
    out_ref[0:HALF, :] = two_three_ref[HALF : 2 * HALF, :]
    for odd in range(2):

        @pl.when(where_ref[2] == odd)
        def _(odd=odd):
            row = (1 - odd) * BLOCK
            out_ref[HALF : HALF + BLOCK, :] = eight_ref[row : row + BLOCK, :]

    out_ref[HALF + BLOCK : HALF + BLOCK + RIDER, :] = two_three_ref[
        2 * HALF + RIDER : 2 * HALF + 2 * RIDER, :
    ]


def total_kernel(four_ref, up_ref, one_ref, seven_ref, two_three_ref, six_five_ref, out_ref):
    at = HALF + BLOCK
    out_ref[0:at, :] = four_ref[0:at, :]
    total = got(up_ref, HALF) + got(one_ref, HALF) + got(seven_ref, HALF)
    total += got(two_three_ref, 2 * HALF) + got(two_three_ref, 2 * HALF + RIDER)
    total += got(six_five_ref, 2 * HALF) + got(four_ref, at)
    put(out_ref, at, total)


def attend_kernel(count, units, tiles, first, last, rider, *refs):
    refs = list(refs)
    where_ref = refs.pop(0)
    if first:
        q_in = [refs.pop(0) for _ in range(2)]
    key_refs = [refs.pop(0) for _ in range(count)]
    state_in = None if first else [refs.pop(0) for _ in range(5)]
    if last:
        out_ref = refs.pop(0)
        q_ref = state_in[0]
        top_ref, sum_ref, mix_ref = refs
    else:
        q_ref, starts_ref, top_ref, sum_ref, mix_ref = refs
    slab, core, odd = where_ref[0], where_ref[1], where_ref[2]
    origin = tiles[0] * 1024 if last else 0

    found_units = []
    for unit in units:
        found = []
        for array, row, distance, partner, rounds in unit:
            base = where_ref[3 + distance] * 512 + (1 - core if partner else core) * 256
            for n, t in enumerate(rounds):
                block = base + (128 if t is None else (odd ^ t) * 128)
                found.append((key_refs[array], row + n * BLOCK, block))
        found_units.append(found)

    one = jnp.full((16, 128), FAR, jnp.float32) if first else state_in[1][0:16, :]
    two = jnp.full((16, 128), FAR, jnp.float32) if first else state_in[1][16:32, :]
    for found in found_units:
        for ref, row, base in found:
            counts = ref[row + 128 : row + BLOCK, :].astype(jnp.float32)
            at = base.astype(jnp.float32)
            n1, n2 = counts[:, :128], counts[:, 128:]
            one = jnp.minimum(one, jnp.where(n1 < 128.0, at + n1, FAR))
            two = jnp.minimum(two, jnp.where(n2 < 128.0, at + n2, FAR))
    if not last:
        starts_ref[0:16, :] = one
        starts_ref[16:32, :] = two
    start1 = jnp.min(one).astype(jnp.int32)
    start2 = jnp.min(two).astype(jnp.int32)

    if first:
        for t in range(2):
            for j in range(8):
                q_ref[t * 1024 + j * 128 : t * 1024 + (j + 1) * 128, :] = q_in[t][
                    0:128, j * HD : (j + 1) * HD
                ]
        top_ref[...] = jnp.full(top_ref.shape, FIRST, jnp.float32)
        sum_ref[...] = jnp.zeros(sum_ref.shape, jnp.float32)
        mix_ref[...] = jnp.zeros(mix_ref.shape, jnp.float32)
    elif last:
        span = slice(origin, origin + 1024)
        top_ref[...] = state_in[2][span, :]
        sum_ref[...] = state_in[3][span, :]
        mix_ref[...] = state_in[4][span, :]

    row_iota = lax.broadcasted_iota(jnp.int32, (128, 128), 0)
    lane_iota = lax.broadcasted_iota(jnp.int32, (128, 128), 1)

    def tile_step(t):
        q_base = slab * 512 + core * 256 + (odd ^ t) * 128

        def low_of(position):
            return jnp.where(
                position >= start2, start2, jnp.where(position >= start1, start1, 0)
            )

        low = low_of(q_base)
        for found in found_units:
            needed = functools.reduce(
                jnp.logical_or,
                [(base <= q_base) & (base + 127 >= low) for ref, row, base in found],
            )

            @pl.when(needed)
            def _(found=found):
                q_pos = q_base + row_iota
                lows = low_of(q_pos)
                allowed = []
                for ref, row, base in found:
                    k_pos = base + lane_iota
                    allowed.append((k_pos >= lows) & (k_pos <= q_pos))
                k = jnp.concatenate([r[row : row + 128, 0:HD] for r, row, _ in found], axis=0)
                v = jnp.concatenate([r[row : row + 128, HD:] for r, row, _ in found], axis=0)
                for pair in range(4):
                    at = t * 1024 + pair * 256
                    q = q_ref[pl.ds(at, 256), :]
                    scores = lax.dot_general(
                        q, k, (((1,), (1,)), ((), ())), preferred_element_type=jnp.float32
                    )
                    parts = []
                    for n, mask in enumerate(allowed):
                        mask2 = jnp.concatenate([mask, mask], axis=0)
                        parts.append(
                            jnp.where(mask2, scores[:, n * 128 : (n + 1) * 128], MASKED)
                        )
                    best = functools.reduce(jnp.maximum, parts)
                    span = pl.ds(at - origin, 256)
                    top_old = top_ref[span, :]
                    top = jnp.maximum(top_old, jnp.max(best, axis=1, keepdims=True))
                    factor = jnp.exp2((top_old - top) * SCALE2)
                    weights = [jnp.exp2((part - top) * SCALE2) for part in parts]
                    sum_ref[span, :] = sum_ref[span, :] * factor + functools.reduce(
                        jnp.add, weights
                    )
                    rounded = jnp.concatenate([w.astype(jnp.bfloat16) for w in weights], axis=1)
                    mix_ref[span, :] = mix_ref[span, :] * factor + jnp.dot(
                        rounded, v, preferred_element_type=jnp.float32
                    )
                    top_ref[span, :] = top

    if len(tiles) == 1:
        tile_step(tiles[0])
    else:

        def loop_step(t, carry):
            tile_step(t)
            return carry

        lax.fori_loop(0, 2, loop_step, 0)
    if last:
        for j in range(8):
            span = slice(j * 128, (j + 1) * 128)
            total = jnp.sum(sum_ref[span, :], axis=1, keepdims=True)
            out_ref[0:128, j * HD : (j + 1) * HD] = (mix_ref[span, :] / total).astype(jnp.bfloat16)
        put_wide(out_ref, got(key_refs[0], rider) + got(key_refs[1], rider))
        out_ref[128:BLOCK, 512:1024] = jnp.zeros((16, 512), jnp.bfloat16)


def finish_kernel(where_ref, first_ref, second_ref, attention_ref, captured_ref, share_ref):
    odd = where_ref[2]
    for swap in range(2):

        @pl.when(odd == swap)
        def _(swap=swap):
            for t, ref in enumerate((first_ref, second_ref)):
                head = t ^ swap
                attention_ref[:, head * 1024 : (head + 1) * 1024] = ref[0:128, :]

    received = [got_wide(first_ref), got_wide(second_ref)]
    row = lax.broadcasted_iota(jnp.int32, (RIDER, 128), 0)
    lane = lax.broadcasted_iota(jnp.int32, (RIDER, 128), 1)
    rows = lax.broadcasted_iota(jnp.int32, (2, 2), 0)
    columns = lax.broadcasted_iota(jnp.int32, (2, 2), 1)
    own, everything = {}, [0.0, 0.0]
    for g in range(2):
        sums = jnp.where(odd == g, received[0], received[1])
        for kind in range(2):
            n = 2 * g + kind
            captured_ref[n] = sums[:, n * RANK : (n + 1) * RANK] * (1.0 / TOKENS)
            here = lane == 64 * (1 - g)
            own[n] = jnp.sum(jnp.where(here & (row == kind), sums, 0.0))
            everything[kind] += 0.5 * jnp.sum(jnp.where(here & (row == kind + 2), sums, 0.0))
    share = jnp.zeros((2, 2), jnp.float32)
    for g in range(2):
        for kind in range(2):
            value = jnp.full((2, 2), KVH * own[2 * g + kind], jnp.float32) / everything[kind]
            share = jnp.where((rows == g) & (columns == kind), value, share)
    share_ref[...] = share


def vmem():
    return pl.BlockSpec(memory_space=pltpu.VMEM)


def smem():
    return pl.BlockSpec(memory_space=pltpu.SMEM)


def rows(count):
    return jax.ShapeDtypeStruct((count, 256), jnp.bfloat16)


def small(kernel, name, out_shape, where, *inputs):
    scalars = [] if where is None else [where]
    return pl.pallas_call(
        kernel,
        out_shape=out_shape,
        in_specs=[smem()] * len(scalars) + [vmem()] * len(inputs),
        out_specs=[vmem()] * len(out_shape),
        compiler_params=pltpu.CompilerParams(vmem_limit_bytes=6 * 1024 * 1024),
        cost_estimate=pl.CostEstimate(flops=1 << 20, bytes_accessed=1 << 18, transcendentals=0),
        name=name,
    )(*scalars, *inputs)


def attend(where, q, arrays, units, state, tile=None, rider=None):
    first, last = state is None, tile is not None
    wide = (2048, 128)
    carry = [
        jax.ShapeDtypeStruct(wide, jnp.bfloat16),
        jax.ShapeDtypeStruct((32, 128), jnp.float32),
        jax.ShapeDtypeStruct(wide, jnp.float32),
        jax.ShapeDtypeStruct(wide, jnp.float32),
        jax.ShapeDtypeStruct(wide, jnp.float32),
    ]
    tiles = (tile,) if last else (0, 1)
    keys = sum(128 * len(piece[4]) for unit in units for piece in unit)
    work = len(tiles) * 1024 * keys
    inputs = (list(q) if first else []) + list(arrays)
    aliases = {}
    if not first:
        if not last:
            aliases = {1 + len(inputs) + n: n for n in range(5)}
        inputs += list(state)
    if last:
        out_shape = [jax.ShapeDtypeStruct((BLOCK, 1024), jnp.bfloat16)]
        scratch = [pltpu.VMEM((1024, 128), jnp.float32)] * 3
    else:
        out_shape, scratch = carry, []
    return list(
        pl.pallas_call(
            functools.partial(attend_kernel, len(arrays), units, tiles, first, last, rider),
            out_shape=out_shape,
            in_specs=[smem()] + [vmem()] * len(inputs),
            out_specs=[vmem()] * len(out_shape),
            scratch_shapes=scratch,
            input_output_aliases=aliases,
            compiler_params=pltpu.CompilerParams(vmem_limit_bytes=16 * 1024 * 1024),
            cost_estimate=pl.CostEstimate(
                flops=4 * work * HD, bytes_accessed=1 << 20, transcendentals=work
            ),
            name="attend_last" if last else "attend",
        )(where, *inputs)
    )


def body(queries, keys, values, segments, basis):
    a, z, y = lax.axis_index("a"), lax.axis_index("z"), lax.axis_index("y")
    c = lax.axis_index("c")
    odd = y & 1
    slab = a * 8 + z
    where = jnp.stack([slab, c, odd] + [(slab - d) % SLABS for d in range(10)]).astype(jnp.int32)

    send0, send1, latents, energy = pl.pallas_call(
        prepare_kernel,
        out_shape=[
            jax.ShapeDtypeStruct((BLOCK, 1280), jnp.bfloat16),
            jax.ShapeDtypeStruct((BLOCK, 1280), jnp.bfloat16),
            jax.ShapeDtypeStruct((128, 128), jnp.bfloat16),
            jax.ShapeDtypeStruct((8, 128), jnp.float32),
        ],
        in_specs=[smem()] + [pl.BlockSpec(memory_space=pltpu.HBM)] * 5,
        out_specs=[vmem()] * 4,
        scratch_shapes=[
            pltpu.VMEM((128, 256), jnp.bfloat16),
            pltpu.VMEM((128, 256), jnp.bfloat16),
            pltpu.VMEM((1, 128), jnp.int32),
            pltpu.VMEM((2, 2, RANK, HD), jnp.bfloat16),
            pltpu.SemaphoreType.DMA((6,)),
        ],
        compiler_params=pltpu.CompilerParams(vmem_limit_bytes=66100000),
        name="prepare",
    )(
        odd.reshape(1).astype(jnp.int32),
        queries,
        keys,
        values,
        segments.reshape(1, 128),
        jnp.swapaxes(basis, 2, 3),
    )
    q = [lax.ppermute(array, COLUMN, to_heads(t)) for t, array in enumerate((send0, send1))]
    energy = added(added(added(energy, "c", 1), "xl", 1), "y", 2)

    def partner(array):
        return lax.ppermute(array, "c", [(0, 1), (1, 0)])

    def after(state, *arrays):
        state[2], *arrays = lax.optimization_barrier((state[2], *arrays))
        return arrays

    def piece(array, row, distance, other):
        return (array, row, distance, other, (None,) if distance == 9 else (0, 1))

    (own,) = small(start_kernel, "start", [rows(HALF + RIDER)], where, *q, energy)
    eight = shifted(own, 8)
    state = attend(where, q, [own], (((piece(0, 0, 0, False)),),), None)

    (eight,) = after(state, eight)
    up, down = small(once_kernel, "once", [rows(HALF + RIDER)] * 2, None, own, eight)
    one, seven = shifted(up, 1), shifted(down, -1)
    state = attend(where, None, [eight], ((piece(0, 0, 8, False),),), state)

    one, seven = after(state, one, seven)
    far_up, far_down = small(
        twice_kernel,
        "twice",
        [rows(2 * HALF + 2 * RIDER), rows(2 * HALF + RIDER)],
        None,
        up,
        one,
        down,
        seven,
    )
    two_three, six_five = shifted(far_up, 2), shifted(far_down, -2)
    other_zero_one, other_eight_seven = partner(far_up), partner(far_down)
    state = attend(
        where, None, [one, seven], ((piece(0, 0, 1, False), piece(1, 0, 7, False)),), state
    )
    state = attend(
        where,
        None,
        [other_zero_one, other_eight_seven],
        (
            (piece(0, 0, 0, True), piece(0, HALF, 1, True)),
            (piece(1, 0, 8, True), piece(1, HALF, 7, True)),
        ),
        state,
    )

    (two_three,) = after(state, two_three)
    (three_tail,) = small(
        tail_kernel, "tail", [rows(HALF + BLOCK + RIDER)], where, two_three, eight
    )
    four = shifted(three_tail, 1)
    other_two_three = partner(two_three)
    state = attend(
        where, None, [two_three], ((piece(0, 0, 2, False), piece(0, HALF, 3, False)),), state
    )

    (six_five,) = after(state, six_five)
    other_six_five = partner(six_five)
    state = attend(
        where,
        None,
        [other_two_three, six_five],
        (
            (piece(0, 0, 2, True), piece(0, HALF, 3, True)),
            (piece(1, 0, 6, False), piece(1, HALF, 5, False)),
        ),
        state,
    )

    (four,) = after(state, four)
    (four,) = small(
        total_kernel,
        "total",
        [rows(HALF + BLOCK + RIDER)],
        None,
        four,
        up,
        one,
        seven,
        two_three,
        six_five,
    )
    other_four = partner(four)
    state = attend(
        where,
        None,
        [other_six_five, four],
        (
            (piece(0, 0, 6, True), piece(0, HALF, 5, True)),
            (piece(1, 0, 4, False), piece(1, HALF, 9, False)),
        ),
        state,
    )
    units = ((piece(0, 0, 4, True), piece(0, HALF, 9, True)),)
    back = []
    for t in range(2):
        (mixed,) = attend(
            where, None, [other_four, four], units, state, tile=t, rider=HALF + BLOCK
        )
        back.append(lax.ppermute(mixed, COLUMN, [(d, s) for s, d in to_heads(t)]))
    attention, captured, share = small(
        finish_kernel,
        "finish",
        [
            jax.ShapeDtypeStruct((128, 2048), jnp.bfloat16),
            jax.ShapeDtypeStruct((4, RANK, RANK), jnp.float32),
            jax.ShapeDtypeStruct((2, 2), jnp.float32),
        ],
        where,
        *back,
    )
    return (attention, latents, captured.reshape(2, 2, RANK, RANK), share)


def solution(mesh):
    torus = Mesh(mesh.devices.reshape(2, 8, 4, 2, 2), ("a", "z", "y", "xl", "c"))
    in_specs = (P(SEQ, KV), P(SEQ, KV), P(SEQ, KV), P(SEQ), P(KV, None, None, None))
    out_specs = (P(SEQ, KV), P(SEQ, KV), P(KV, None, None, None), P(KV, None))
    return jax.shard_map(body, mesh=torus, in_specs=in_specs, out_specs=out_specs, check_vma=False)
```

```python
import functools
import math

import jax
import jax.numpy as jnp
from jax import lax
from jax.experimental import pallas as pl
from jax.experimental.pallas import tpu as pltpu
from jax.sharding import Mesh
from jax.sharding import PartitionSpec as P

HD = 128
KVH = 8
RANK = 32
TOKENS = 8192
SLABS = 16
SEQ = ("a", "z", "y")
KV = ("xl", "c")
RING = ("a", "z")
COLUMN = ("y", "c")
BLOCK = 144
HALF = 2 * BLOCK
RIDER = 32
SCALE2 = HD**-0.5 * math.log2(math.e)
FIRST = -1e30
MASKED = -2e30
FAR = 1e9


def to_heads(t):
    pairs = []
    for y in range(4):
        for c in range(2):
            head = (y & 1) ^ t
            pairs.append((y * 2 + c, (2 * c + head) * 2 + (y >> 1)))
    return pairs


def shifted(array, by):
    return lax.ppermute(array, RING, [(i, (i + by) % SLABS) for i in range(SLABS)])


def added(array, axis, distance):
    size = lax.axis_size(axis)
    return array + lax.ppermute(array, axis, [(i, i ^ distance) for i in range(size)])


def place():
    slab = lax.axis_index("a") * 8 + lax.axis_index("z")
    return slab, lax.axis_index("c"), lax.axis_index("y") & 1


def encoded(total):
    high = total.astype(jnp.bfloat16)
    rest = (total - high.astype(jnp.float32)).astype(jnp.bfloat16)
    return high, rest


def put(ref, row, total):
    ref[row : row + RIDER, 0:128], ref[row : row + RIDER, 128:256] = encoded(total)


def got(ref, row):
    rows = slice(row, row + RIDER)
    return ref[rows, 0:128].astype(jnp.float32) + ref[rows, 128:256].astype(jnp.float32)


def put_wide(ref, total):
    for n, part in enumerate(encoded(total)):
        for m in range(2):
            lanes = slice(m * 256 + n * 128, m * 256 + n * 128 + 128)
            ref[128:BLOCK, lanes] = part[m * 16 : (m + 1) * 16, :]


def got_wide(ref):
    rows = []
    for m in range(2):
        high = ref[128:BLOCK, m * 256 : m * 256 + 128].astype(jnp.float32)
        rest = ref[128:BLOCK, m * 256 + 128 : m * 256 + 256].astype(jnp.float32)
        rows.append(high + rest)
    return jnp.concatenate(rows, axis=0)


def prepare_kernel(
    keys_hbm,
    values_hbm,
    segments_hbm,
    basis_hbm,
    first_ref,
    second_ref,
    latents_ref,
    energy_ref,
    keys_ref,
    values_ref,
    segments_ref,
    basis_ref,
    semaphores,
):
    loads = [
        pltpu.make_async_copy(source, target, semaphores.at[n])
        for n, (source, target) in enumerate(
            (
                (segments_hbm, segments_ref),
                (keys_hbm, keys_ref),
                (values_hbm, values_ref),
                (basis_hbm, basis_ref),
            )
        )
    ]
    for copy in loads:
        copy.start()
    for copy in loads:
        copy.wait()
    ids = segments_ref[...]
    n1 = jnp.sum((ids < 1).astype(jnp.float32))
    n2 = jnp.sum((ids < 2).astype(jnp.float32))
    lanes = lax.broadcasted_iota(jnp.int32, (16, 256), 1)
    counts = jnp.where(lanes < 128, n1, n2).astype(jnp.bfloat16)
    projected, energies = [], []
    for g in range(2):
        for kind, ref in enumerate((keys_ref, values_ref)):
            rows = ref[:, g * HD : (g + 1) * HD]
            projected.append(
                lax.dot_general(
                    rows,
                    basis_ref[g, kind],
                    (((1,), (1,)), ((), ())),
                    preferred_element_type=jnp.float32,
                )
            )
            squares = rows.astype(jnp.float32)
            energies.append(jnp.sum(squares * squares))
    latents = jnp.concatenate(projected, axis=1)
    latents_ref[...] = latents.astype(jnp.bfloat16)
    seen = lax.dot_general(
        latents,
        latents,
        (((0,), (0,)), ((), ())),
        precision=lax.Precision.HIGHEST,
        preferred_element_type=jnp.float32,
    )
    lane = lax.broadcasted_iota(jnp.int32, (RIDER, 128), 1) // RANK
    row = lax.broadcasted_iota(jnp.int32, (RIDER, 128), 0)
    riders = []
    for g in range(2):
        other = jnp.where(row == 0, energies[2 * g], jnp.where(row == 1, energies[2 * g + 1], 0.0))
        for n in (2 * g, 2 * g + 1):
            other = jnp.where(lane == n, seen[n * RANK : (n + 1) * RANK, :], other)
        riders.append(other)
    row8 = lax.broadcasted_iota(jnp.int32, (8, 128), 0)
    energy_ref[...] = jnp.where(
        row8 == 0,
        energies[0] + energies[2],
        jnp.where(row8 == 1, energies[1] + energies[3], 0.0),
    )
    for odd in range(2):

        @pl.when(place()[2] == odd)
        def _(odd=odd):
            for ref, head in ((first_ref, odd), (second_ref, 1 - odd)):
                ref[0:128, 0:HD] = keys_ref[:, head * HD : (head + 1) * HD]
                ref[0:128, HD : 2 * HD] = values_ref[:, head * HD : (head + 1) * HD]
                put(ref, BLOCK, riders[head])

    for ref in (first_ref, second_ref):
        ref[128:BLOCK, :] = counts


def start_kernel(first_ref, second_ref, energy_ref, out_ref):
    out_ref[0:BLOCK, :] = first_ref[0:BLOCK, :]
    out_ref[BLOCK:HALF, :] = second_ref[0:BLOCK, :]
    lane = lax.broadcasted_iota(jnp.int32, (RIDER, 128), 1) // 64
    row = lax.broadcasted_iota(jnp.int32, (RIDER, 128), 0)
    energy = jnp.where(
        row == 2, energy_ref[0:1, :], jnp.where(row == 3, energy_ref[1:2, :], 0.0)
    )
    energy = jnp.where(lane == 1 - place()[2], energy, 0.0)
    put(out_ref, HALF, got(first_ref, BLOCK) + got(second_ref, BLOCK) + energy)


def once_kernel(own_ref, eight_ref, up_ref, down_ref):
    both = got(own_ref, HALF) + got(eight_ref, HALF)
    up_ref[0:HALF, :] = own_ref[0:HALF, :]
    down_ref[0:HALF, :] = eight_ref[0:HALF, :]
    put(up_ref, HALF, both)
    put(down_ref, HALF, both)


def twice_kernel(up_ref, one_ref, down_ref, seven_ref, far_up_ref, far_down_ref):
    far_up_ref[0:HALF, :] = up_ref[0:HALF, :]
    far_up_ref[HALF : 2 * HALF, :] = one_ref[0:HALF, :]
    far_up_ref[2 * HALF : 2 * HALF + RIDER, :] = up_ref[HALF : HALF + RIDER, :]
    far_up_ref[2 * HALF + RIDER : 2 * HALF + 2 * RIDER, :] = one_ref[HALF : HALF + RIDER, :]
    far_down_ref[0:HALF, :] = down_ref[0:HALF, :]
    far_down_ref[HALF : 2 * HALF, :] = seven_ref[0:HALF, :]
    put(far_down_ref, 2 * HALF, got(down_ref, HALF) + got(seven_ref, HALF))


def tail_kernel(two_three_ref, eight_ref, out_ref):
    out_ref[0:HALF, :] = two_three_ref[HALF : 2 * HALF, :]
    for odd in range(2):

        @pl.when(place()[2] == odd)
        def _(odd=odd):
            row = (1 - odd) * BLOCK
            out_ref[HALF : HALF + BLOCK, :] = eight_ref[row : row + BLOCK, :]

    out_ref[HALF + BLOCK : HALF + BLOCK + RIDER, :] = two_three_ref[
        2 * HALF + RIDER : 2 * HALF + 2 * RIDER, :
    ]


def total_kernel(four_ref, up_ref, one_ref, seven_ref, two_three_ref, six_five_ref, out_ref, energy_ref):
    at = HALF + BLOCK
    out_ref[0:at, :] = four_ref[0:at, :]
    total = got(up_ref, HALF) + got(one_ref, HALF) + got(seven_ref, HALF)
    total += got(two_three_ref, 2 * HALF) + got(two_three_ref, 2 * HALF + RIDER)
    total += got(six_five_ref, 2 * HALF) + got(four_ref, at)
    put(out_ref, at, total)
    lane = lax.broadcasted_iota(jnp.int32, (RIDER, 128), 1) // 64
    row = lax.broadcasted_iota(jnp.int32, (RIDER, 128), 0)
    energies = (lane == 1 - place()[2]) & ((row == 2) | (row == 3))
    energy_ref[...] = jnp.where(energies, 2.0 * total, 0.0)


def attend_kernel(count, units, tiles, first, last, rider, *refs):
    refs = list(refs)
    if first:
        q_in = [refs.pop(0) for _ in range(2)]
    key_refs = [refs.pop(0) for _ in range(count)]
    state_in = None if first else [refs.pop(0) for _ in range(5)]
    if last:
        energy_ref = refs.pop(0)
        out_ref = refs.pop(0)
        q_ref = state_in[0]
        top_ref, sum_ref, mix_ref = refs
    else:
        q_ref, starts_ref, top_ref, sum_ref, mix_ref = refs
    slab, core, odd = place()
    origin = tiles[0] * 1024 if last else 0

    found_units = []
    for unit in units:
        found = []
        for array, row, distance, partner, rounds in unit:
            base = ((slab - distance) & (SLABS - 1)) * 512 + (1 - core if partner else core) * 256
            for n, t in enumerate(rounds):
                block = base + (128 if t is None else (odd ^ t) * 128)
                found.append((key_refs[array], row + n * BLOCK, block))
        found_units.append(found)

    one = jnp.full((16, 128), FAR, jnp.float32) if first else state_in[1][0:16, :]
    two = jnp.full((16, 128), FAR, jnp.float32) if first else state_in[1][16:32, :]
    for found in found_units:
        for ref, row, base in found:
            counts = ref[row + 128 : row + BLOCK, :].astype(jnp.float32)
            at = base.astype(jnp.float32)
            n1, n2 = counts[:, :128], counts[:, 128:]
            one = jnp.minimum(one, jnp.where(n1 < 128.0, at + n1, FAR))
            two = jnp.minimum(two, jnp.where(n2 < 128.0, at + n2, FAR))
    if not last:
        starts_ref[0:16, :] = one
        starts_ref[16:32, :] = two
    start1 = jnp.min(one).astype(jnp.int32)
    start2 = jnp.min(two).astype(jnp.int32)

    if first:
        for t in range(2):
            for j in range(8):
                q_ref[t * 1024 + j * 128 : t * 1024 + (j + 1) * 128, :] = q_in[t][
                    0:128, j * HD : (j + 1) * HD
                ]
        top_ref[...] = jnp.full(top_ref.shape, FIRST, jnp.float32)
        sum_ref[...] = jnp.zeros(sum_ref.shape, jnp.float32)
        mix_ref[...] = jnp.zeros(mix_ref.shape, jnp.float32)
    elif last:
        span = slice(origin, origin + 1024)
        top_ref[...] = state_in[2][span, :]
        sum_ref[...] = state_in[3][span, :]
        mix_ref[...] = state_in[4][span, :]

    row_iota = lax.broadcasted_iota(jnp.int32, (128, 128), 0)
    lane_iota = lax.broadcasted_iota(jnp.int32, (128, 128), 1)

    def low_of(position):
        return jnp.where(position >= start2, start2, jnp.where(position >= start1, start1, 0))

    q_base = {t: slab * 512 + core * 256 + (odd ^ t) * 128 for t in tiles}
    for found in found_units:
        needed = functools.reduce(
            jnp.logical_or,
            [
                (base <= q_base[t]) & (base + 127 >= low_of(q_base[t]))
                for t in tiles
                for ref, row, base in found
            ],
        )

        @pl.when(needed)
        def _(found=found):
            k = jnp.concatenate([r[row : row + 128, 0:HD] for r, row, _ in found], axis=0)
            v = jnp.concatenate([r[row : row + 128, HD : 2 * HD] for r, row, _ in found], axis=0)
            scores = {
                t: lax.dot_general(
                    q_ref[t * 1024 : (t + 1) * 1024, :],
                    k,
                    (((1,), (1,)), ((), ())),
                    preferred_element_type=jnp.float32,
                )
                for t in tiles
            }
            for t in tiles:
                q_pos = q_base[t] + row_iota
                lows = low_of(q_pos)
                parts = []
                for n, (ref, row, base) in enumerate(found):
                    k_pos = base + lane_iota
                    mask = (k_pos >= lows) & (k_pos <= q_pos)
                    mask = jnp.concatenate([mask] * 8, axis=0)
                    parts.append(
                        jnp.where(mask, scores[t][:, n * 128 : (n + 1) * 128], MASKED)
                    )
                best = functools.reduce(jnp.maximum, parts)
                span = slice(t * 1024 - origin, (t + 1) * 1024 - origin)
                top_old = top_ref[span, :]
                top = jnp.maximum(top_old, jnp.max(best, axis=1, keepdims=True))
                factor = jnp.exp2((top_old - top) * SCALE2)
                weights = [jnp.exp2((part - top) * SCALE2) for part in parts]
                sum_ref[span, :] = sum_ref[span, :] * factor + functools.reduce(jnp.add, weights)
                rounded = jnp.concatenate([w.astype(jnp.bfloat16) for w in weights], axis=1)
                mix_ref[span, :] = mix_ref[span, :] * factor + jnp.dot(
                    rounded, v, preferred_element_type=jnp.float32
                )
                top_ref[span, :] = top

    if last:
        for j in range(8):
            span = slice(j * 128, (j + 1) * 128)
            total = jnp.sum(sum_ref[span, :], axis=1, keepdims=True)
            out_ref[0:128, j * HD : (j + 1) * HD] = (mix_ref[span, :] / total).astype(jnp.bfloat16)
        total = got(key_refs[0], rider) + got(key_refs[1], rider) + energy_ref[...]
        put_wide(out_ref, total)
        out_ref[128:BLOCK, 512:1024] = jnp.zeros((16, 512), jnp.bfloat16)


def finish_kernel(first_ref, second_ref, attention_ref, captured_ref, share_ref):
    odd = place()[2]
    for swap in range(2):

        @pl.when(odd == swap)
        def _(swap=swap):
            for t, ref in enumerate((first_ref, second_ref)):
                head = t ^ swap
                attention_ref[:, head * 1024 : (head + 1) * 1024] = ref[0:128, :]

    received = [got_wide(first_ref), got_wide(second_ref)]
    row = lax.broadcasted_iota(jnp.int32, (RIDER, 128), 0)
    lane = lax.broadcasted_iota(jnp.int32, (RIDER, 128), 1)
    rows = lax.broadcasted_iota(jnp.int32, (2, 2), 0)
    columns = lax.broadcasted_iota(jnp.int32, (2, 2), 1)
    own, everything = {}, [0.0, 0.0]
    for g in range(2):
        sums = jnp.where(odd == g, received[0], received[1])
        for kind in range(2):
            n = 2 * g + kind
            captured_ref[n] = sums[:, n * RANK : (n + 1) * RANK] * (1.0 / TOKENS)
            here = lane == 64 * (1 - g)
            own[n] = jnp.sum(jnp.where(here & (row == kind), sums, 0.0))
            everything[kind] += 0.5 * jnp.sum(jnp.where(here & (row == kind + 2), sums, 0.0))
    share = jnp.zeros((2, 2), jnp.float32)
    for g in range(2):
        for kind in range(2):
            value = jnp.full((2, 2), KVH * own[2 * g + kind], jnp.float32) / everything[kind]
            share = jnp.where((rows == g) & (columns == kind), value, share)
    share_ref[...] = share


def vmem():
    return pl.BlockSpec(memory_space=pltpu.VMEM)


def rows(count):
    return jax.ShapeDtypeStruct((count, 256), jnp.bfloat16)


def small(kernel, out_shape, *inputs):
    return pl.pallas_call(
        kernel,
        out_shape=out_shape,
        in_specs=[vmem()] * len(inputs),
        out_specs=[vmem()] * len(out_shape),
        compiler_params=pltpu.CompilerParams(vmem_limit_bytes=6 * 1024 * 1024),
        cost_estimate=pl.CostEstimate(flops=1 << 20, bytes_accessed=1 << 18, transcendentals=0),
    )(*inputs)


def attend(q, arrays, units, state, tile=None, rider=None, energy=None):
    first, last = state is None, tile is not None
    wide = (2048, 128)
    carry = [
        jax.ShapeDtypeStruct(wide, jnp.bfloat16),
        jax.ShapeDtypeStruct((32, 128), jnp.float32),
        jax.ShapeDtypeStruct(wide, jnp.float32),
        jax.ShapeDtypeStruct(wide, jnp.float32),
        jax.ShapeDtypeStruct(wide, jnp.float32),
    ]
    tiles = (tile,) if last else (0, 1)
    keys = sum(128 * len(piece[4]) for unit in units for piece in unit)
    work = len(tiles) * 1024 * keys
    inputs = (list(q) if first else []) + list(arrays)
    aliases = {}
    if not first:
        if not last:
            aliases = {len(inputs) + n: n for n in range(5)}
        inputs += list(state)
    if last:
        inputs.append(energy)
        out_shape = [jax.ShapeDtypeStruct((BLOCK, 1024), jnp.bfloat16)]
        scratch = [pltpu.VMEM((1024, 128), jnp.float32)] * 3
    else:
        out_shape, scratch = carry, []
    return list(
        pl.pallas_call(
            functools.partial(attend_kernel, len(arrays), units, tiles, first, last, rider),
            out_shape=out_shape,
            in_specs=[vmem()] * len(inputs),
            out_specs=[vmem()] * len(out_shape),
            scratch_shapes=scratch,
            input_output_aliases=aliases,
            compiler_params=pltpu.CompilerParams(vmem_limit_bytes=20 * 1024 * 1024),
            cost_estimate=pl.CostEstimate(
                flops=4 * work * HD, bytes_accessed=1 << 20, transcendentals=work
            ),
            name="attend_last" if last else "attend",
        )(*inputs)
    )


def body(queries, keys, values, segments, basis):
    odd = lax.axis_index("y") & 1
    send0, send1, latents, energy = pl.pallas_call(
        prepare_kernel,
        out_shape=[
            rows(BLOCK + RIDER),
            rows(BLOCK + RIDER),
            jax.ShapeDtypeStruct((128, 128), jnp.bfloat16),
            jax.ShapeDtypeStruct((8, 128), jnp.float32),
        ],
        in_specs=[pl.BlockSpec(memory_space=pltpu.HBM)] * 4,
        out_specs=[vmem()] * 4,
        scratch_shapes=[
            pltpu.VMEM((128, 256), jnp.bfloat16),
            pltpu.VMEM((128, 256), jnp.bfloat16),
            pltpu.VMEM((1, 128), jnp.int32),
            pltpu.VMEM((2, 2, RANK, HD), jnp.bfloat16),
            pltpu.SemaphoreType.DMA((4,)),
        ],
        compiler_params=pltpu.CompilerParams(vmem_limit_bytes=66100000),
        name="prepare",
    )(keys, values, segments.reshape(1, 128), jnp.swapaxes(basis, 2, 3))
    kv = [lax.ppermute(array, COLUMN, to_heads(t)) for t, array in enumerate((send0, send1))]
    slices = [lax.dynamic_slice_in_dim(queries, (odd ^ t) * 1024, 1024, 1) for t in range(2)]
    q = []
    for t in range(2):
        q.append(lax.ppermute(slices[t], COLUMN, to_heads(t)))
    *kv, _, _ = lax.optimization_barrier((*kv, *slices))
    energy = added(added(energy, "c", 1), "xl", 1)

    def partner(array):
        return lax.ppermute(array, "c", [(0, 1), (1, 0)])

    def after(state, *arrays):
        state[2], *arrays = lax.optimization_barrier((state[2], *arrays))
        return arrays

    def piece(array, row, distance, other):
        return (array, row, distance, other, (None,) if distance == 9 else (0, 1))

    (own,) = small(start_kernel, [rows(HALF + RIDER)], *kv, energy)
    eight = shifted(own, 8)
    up, down = small(once_kernel, [rows(HALF + RIDER)] * 2, own, eight)
    one, seven = shifted(up, 1), shifted(down, -1)
    state = attend(
        q, [own, eight], ((piece(0, 0, 0, False), piece(1, 0, 8, False)),), None
    )

    one, seven = after(state, one, seven)
    far_up, far_down = small(
        twice_kernel, [rows(2 * HALF + 2 * RIDER), rows(2 * HALF + RIDER)], up, one, down, seven
    )
    two_three, six_five = shifted(far_up, 2), shifted(far_down, -2)
    other_zero_one, other_eight_seven = partner(far_up), partner(far_down)
    state = attend(
        None, [one, seven], ((piece(0, 0, 1, False), piece(1, 0, 7, False)),), state
    )
    state = attend(
        None,
        [other_zero_one, other_eight_seven],
        (
            (piece(0, 0, 0, True), piece(0, HALF, 1, True)),
            (piece(1, 0, 8, True), piece(1, HALF, 7, True)),
        ),
        state,
    )

    (two_three,) = after(state, two_three)
    (three_tail,) = small(tail_kernel, [rows(HALF + BLOCK + RIDER)], two_three, eight)
    four = shifted(three_tail, 1)
    other_two_three = partner(two_three)
    state = attend(
        None, [two_three], ((piece(0, 0, 2, False), piece(0, HALF, 3, False)),), state
    )

    (six_five,) = after(state, six_five)
    other_six_five = partner(six_five)
    state = attend(
        None,
        [other_two_three, six_five],
        (
            (piece(0, 0, 2, True), piece(0, HALF, 3, True)),
            (piece(1, 0, 6, False), piece(1, HALF, 5, False)),
        ),
        state,
    )

    (four,) = after(state, four)
    four, energy = small(
        total_kernel,
        [rows(HALF + BLOCK + RIDER), jax.ShapeDtypeStruct((RIDER, 128), jnp.float32)],
        four,
        up,
        one,
        seven,
        two_three,
        six_five,
    )
    other_four = partner(four)
    energy = lax.ppermute(energy, "y", [(i, i ^ 2) for i in range(4)])
    state = attend(
        None, [other_six_five], ((piece(0, 0, 6, True), piece(0, HALF, 5, True)),), state
    )
    units = (
        (piece(1, 0, 4, False), piece(1, HALF, 9, False)),
        (piece(0, 0, 4, True), piece(0, HALF, 9, True)),
    )
    back = []
    for t in range(2):
        (mixed,) = attend(
            None, [other_four, four], units, state, t, HALF + BLOCK, energy
        )
        back.append(lax.ppermute(mixed, COLUMN, [(d, s) for s, d in to_heads(t)]))
    attention, captured, share = small(
        finish_kernel,
        [
            jax.ShapeDtypeStruct((128, 2048), jnp.bfloat16),
            jax.ShapeDtypeStruct((4, RANK, RANK), jnp.float32),
            jax.ShapeDtypeStruct((2, 2), jnp.float32),
        ],
        *back,
    )
    return (attention, latents, captured.reshape(2, 2, RANK, RANK), share)


def solution(mesh):
    torus = Mesh(mesh.devices.reshape(2, 8, 4, 2, 2), ("a", "z", "y", "xl", "c"))
    in_specs = (P(SEQ, KV), P(SEQ, KV), P(SEQ, KV), P(SEQ), P(KV, None, None, None))
    out_specs = (P(SEQ, KV), P(SEQ, KV), P(KV, None, None, None), P(KV, None))

    return jax.shard_map(body, mesh=torus, in_specs=in_specs, out_specs=out_specs, check_vma=False)
```

```python
import functools
import math

import jax
import jax.numpy as jnp
from jax import lax
from jax.experimental import pallas as pl
from jax.experimental.pallas import tpu as pltpu
from jax.sharding import Mesh
from jax.sharding import PartitionSpec as P

HD = 128
KVH = 8
RANK = 32
TOKENS = 8192
SLABS = 16
SEQ = ("a", "z", "y")
KV = ("xl", "c")
RING = ("a", "z")
COLUMN = ("y", "c")
BLOCK = 144
HALF = 2 * BLOCK
RIDER = 32
SCALE2 = HD**-0.5 * math.log2(math.e)
FIRST = -1e30
MASKED = -2e30
FAR = 1e9


def to_heads(t):
    pairs = []
    for y in range(4):
        for c in range(2):
            head = (y & 1) ^ t
            pairs.append((y * 2 + c, (2 * c + head) * 2 + (y >> 1)))
    return pairs


def shifted(array, by):
    return lax.ppermute(array, RING, [(i, (i + by) % SLABS) for i in range(SLABS)])


def added(array, axis, distance):
    size = lax.axis_size(axis)
    return array + lax.ppermute(array, axis, [(i, i ^ distance) for i in range(size)])


def place():
    slab = lax.axis_index("a") * 8 + lax.axis_index("z")
    return slab, lax.axis_index("c"), lax.axis_index("y") & 1


def encoded(total):
    high = total.astype(jnp.bfloat16)
    rest = (total - high.astype(jnp.float32)).astype(jnp.bfloat16)
    return high, rest


def put(ref, row, total):
    ref[row : row + RIDER, 0:128], ref[row : row + RIDER, 128:256] = encoded(total)


def got(ref, row):
    rows = slice(row, row + RIDER)
    return ref[rows, 0:128].astype(jnp.float32) + ref[rows, 128:256].astype(jnp.float32)


def put_wide(ref, total):
    for n, part in enumerate(encoded(total)):
        for m in range(2):
            lanes = slice(m * 256 + n * 128, m * 256 + n * 128 + 128)
            ref[128:BLOCK, lanes] = part[m * 16 : (m + 1) * 16, :]


def got_wide(ref):
    rows = []
    for m in range(2):
        high = ref[128:BLOCK, m * 256 : m * 256 + 128].astype(jnp.float32)
        rest = ref[128:BLOCK, m * 256 + 128 : m * 256 + 256].astype(jnp.float32)
        rows.append(high + rest)
    return jnp.concatenate(rows, axis=0)


def prepare_kernel(
    keys_hbm,
    values_hbm,
    segments_hbm,
    basis_hbm,
    first_ref,
    second_ref,
    latents_ref,
    energy_ref,
    keys_ref,
    values_ref,
    segments_ref,
    basis_ref,
    semaphores,
):
    loads = [
        pltpu.make_async_copy(source, target, semaphores.at[n])
        for n, (source, target) in enumerate(
            (
                (segments_hbm, segments_ref),
                (keys_hbm, keys_ref),
                (values_hbm, values_ref),
                (basis_hbm, basis_ref),
            )
        )
    ]
    for copy in loads:
        copy.start()
    for copy in loads:
        copy.wait()
    ids = segments_ref[...]
    n1 = jnp.sum((ids < 1).astype(jnp.float32))
    n2 = jnp.sum((ids < 2).astype(jnp.float32))
    lanes = lax.broadcasted_iota(jnp.int32, (16, 256), 1)
    counts = jnp.where(lanes < 128, n1, n2).astype(jnp.bfloat16)
    projected, energies = [], []
    for g in range(2):
        for kind, ref in enumerate((keys_ref, values_ref)):
            rows = ref[:, g * HD : (g + 1) * HD]
            projected.append(
                lax.dot_general(
                    rows,
                    basis_ref[g, kind],
                    (((1,), (1,)), ((), ())),
                    preferred_element_type=jnp.float32,
                )
            )
            squares = rows.astype(jnp.float32)
            energies.append(jnp.sum(squares * squares))
    latents = jnp.concatenate(projected, axis=1)
    latents_ref[...] = latents.astype(jnp.bfloat16)
    seen = lax.dot_general(
        latents,
        latents,
        (((0,), (0,)), ((), ())),
        precision=lax.Precision.HIGHEST,
        preferred_element_type=jnp.float32,
    )
    lane = lax.broadcasted_iota(jnp.int32, (RIDER, 128), 1) // RANK
    row = lax.broadcasted_iota(jnp.int32, (RIDER, 128), 0)
    riders = []
    for g in range(2):
        other = jnp.where(row == 0, energies[2 * g], jnp.where(row == 1, energies[2 * g + 1], 0.0))
        for n in (2 * g, 2 * g + 1):
            other = jnp.where(lane == n, seen[n * RANK : (n + 1) * RANK, :], other)
        riders.append(other)
    row8 = lax.broadcasted_iota(jnp.int32, (8, 128), 0)
    energy_ref[...] = jnp.where(
        row8 == 0,
        energies[0] + energies[2],
        jnp.where(row8 == 1, energies[1] + energies[3], 0.0),
    )
    for odd in range(2):

        @pl.when(place()[2] == odd)
        def _(odd=odd):
            for ref, head in ((first_ref, odd), (second_ref, 1 - odd)):
                ref[0:128, 0:HD] = keys_ref[:, head * HD : (head + 1) * HD]
                ref[0:128, HD : 2 * HD] = values_ref[:, head * HD : (head + 1) * HD]
                put(ref, BLOCK, riders[head])

    for ref in (first_ref, second_ref):
        ref[128:BLOCK, :] = counts


def start_kernel(first_ref, second_ref, energy_ref, out_ref):
    out_ref[0:BLOCK, :] = first_ref[0:BLOCK, :]
    out_ref[BLOCK:HALF, :] = second_ref[0:BLOCK, :]
    lane = lax.broadcasted_iota(jnp.int32, (RIDER, 128), 1) // 64
    row = lax.broadcasted_iota(jnp.int32, (RIDER, 128), 0)
    energy = jnp.where(
        row == 2, energy_ref[0:1, :], jnp.where(row == 3, energy_ref[1:2, :], 0.0)
    )
    energy = jnp.where(lane == 1 - place()[2], energy, 0.0)
    put(out_ref, HALF, got(first_ref, BLOCK) + got(second_ref, BLOCK) + energy)


def once_kernel(own_ref, eight_ref, up_ref, down_ref, both_ref):
    both = got(own_ref, HALF) + got(eight_ref, HALF)
    up_ref[0:HALF, :] = own_ref[0:HALF, :]
    down_ref[0:HALF, :] = eight_ref[0:HALF, :]
    put(up_ref, HALF, both)
    put(down_ref, HALF, both)
    for odd in range(2):

        @pl.when(place()[2] == odd)
        def _(odd=odd):
            row = (1 - odd) * BLOCK
            up_ref[HALF + RIDER : HALF + RIDER + BLOCK, :] = eight_ref[row : row + BLOCK, :]

    both_ref[0:HALF, :] = own_ref[0:HALF, :]
    both_ref[HALF : 2 * HALF, :] = eight_ref[0:HALF, :]


def split_kernel(one_ref, seven_ref, next_ref, both_ref):
    next_ref[...] = one_ref[0 : HALF + RIDER, :]
    both_ref[0:HALF, :] = one_ref[0:HALF, :]
    both_ref[HALF : 2 * HALF, :] = seven_ref[0:HALF, :]
    both_ref[2 * HALF : 2 * HALF + BLOCK, :] = one_ref[HALF + RIDER : HALF + RIDER + BLOCK, :]


def pair_kernel(first_ref, second_ref, both_ref):
    both_ref[0:HALF, :] = first_ref[0:HALF, :]
    both_ref[HALF : 2 * HALF, :] = second_ref[0:HALF, :]


def total_kernel(*refs):
    *terms, out_ref, energy_ref = refs
    out_ref[0:HALF, :] = terms[0][0:HALF, :]
    total = functools.reduce(jnp.add, [got(ref, HALF) for ref in terms])
    put(out_ref, HALF, total)
    lane = lax.broadcasted_iota(jnp.int32, (RIDER, 128), 1) // 64
    row = lax.broadcasted_iota(jnp.int32, (RIDER, 128), 0)
    energies = (lane == 1 - place()[2]) & ((row == 2) | (row == 3))
    energy_ref[...] = jnp.where(energies, 2.0 * total, 0.0)


def attend_kernel(count, units, tiles, first, last, rider, *refs):
    refs = list(refs)
    if first:
        q_in = [refs.pop(0) for _ in range(2)]
    key_refs = [refs.pop(0) for _ in range(count)]
    state_in = None if first else [refs.pop(0) for _ in range(5)]
    if last:
        energy_ref = refs.pop(0)
        out_ref = refs.pop(0)
        q_ref = state_in[0]
        top_ref, sum_ref, mix_ref = refs
    else:
        q_ref, starts_ref, top_ref, sum_ref, mix_ref = refs
    slab, core, odd = place()
    origin = tiles[0] * 1024 if last else 0

    found_units = []
    for unit in units:
        found = []
        for array, row, distance, partner, rounds in unit:
            base = ((slab - distance) & (SLABS - 1)) * 512 + (1 - core if partner else core) * 256
            for n, t in enumerate(rounds):
                block = base + (128 if t is None else (odd ^ t) * 128)
                found.append((key_refs[array], row + n * BLOCK, block))
        found_units.append(found)

    one = jnp.full((16, 128), FAR, jnp.float32) if first else state_in[1][0:16, :]
    two = jnp.full((16, 128), FAR, jnp.float32) if first else state_in[1][16:32, :]
    for found in found_units:
        for ref, row, base in found:
            counts = ref[row + 128 : row + BLOCK, :].astype(jnp.float32)
            at = base.astype(jnp.float32)
            n1, n2 = counts[:, :128], counts[:, 128:]
            one = jnp.minimum(one, jnp.where(n1 < 128.0, at + n1, FAR))
            two = jnp.minimum(two, jnp.where(n2 < 128.0, at + n2, FAR))
    if not last:
        starts_ref[0:16, :] = one
        starts_ref[16:32, :] = two
    start1 = jnp.min(one).astype(jnp.int32)
    start2 = jnp.min(two).astype(jnp.int32)

    if first:
        for t in range(2):
            for j in range(8):
                q_ref[t * 1024 + j * 128 : t * 1024 + (j + 1) * 128, :] = q_in[t][
                    0:128, j * HD : (j + 1) * HD
                ]
        top_ref[...] = jnp.full(top_ref.shape, FIRST, jnp.float32)
        sum_ref[...] = jnp.zeros(sum_ref.shape, jnp.float32)
        mix_ref[...] = jnp.zeros(mix_ref.shape, jnp.float32)
    elif last:
        span = slice(origin, origin + 1024)
        top_ref[...] = state_in[2][span, :]
        sum_ref[...] = state_in[3][span, :]
        mix_ref[...] = state_in[4][span, :]

    row_iota = lax.broadcasted_iota(jnp.int32, (128, 128), 0)
    lane_iota = lax.broadcasted_iota(jnp.int32, (128, 128), 1)

    def low_of(position):
        return jnp.where(position >= start2, start2, jnp.where(position >= start1, start1, 0))

    q_base = {t: slab * 512 + core * 256 + (odd ^ t) * 128 for t in tiles}
    for found in found_units:
        needed = functools.reduce(
            jnp.logical_or,
            [
                (base <= q_base[t]) & (base + 127 >= low_of(q_base[t]))
                for t in tiles
                for ref, row, base in found
            ],
        )

        @pl.when(needed)
        def _(found=found):
            k = jnp.concatenate([r[row : row + 128, 0:HD] for r, row, _ in found], axis=0)
            v = jnp.concatenate([r[row : row + 128, HD : 2 * HD] for r, row, _ in found], axis=0)
            scores = {
                t: lax.dot_general(
                    q_ref[t * 1024 : (t + 1) * 1024, :],
                    k,
                    (((1,), (1,)), ((), ())),
                    preferred_element_type=jnp.float32,
                )
                for t in tiles
            }
            for t in tiles:
                q_pos = q_base[t] + row_iota
                lows = low_of(q_pos)
                parts = []
                for n, (ref, row, base) in enumerate(found):
                    k_pos = base + lane_iota
                    mask = (k_pos >= lows) & (k_pos <= q_pos)
                    mask = jnp.concatenate([mask] * 8, axis=0)
                    parts.append(
                        jnp.where(mask, scores[t][:, n * 128 : (n + 1) * 128], MASKED)
                    )
                best = functools.reduce(jnp.maximum, parts)
                span = slice(t * 1024 - origin, (t + 1) * 1024 - origin)
                top_old = top_ref[span, :]
                top = jnp.maximum(top_old, jnp.max(best, axis=1, keepdims=True))
                factor = jnp.exp2((top_old - top) * SCALE2)
                weights = [jnp.exp2((part - top) * SCALE2) for part in parts]
                sum_ref[span, :] = sum_ref[span, :] * factor + functools.reduce(jnp.add, weights)
                rounded = jnp.concatenate([w.astype(jnp.bfloat16) for w in weights], axis=1)
                mix_ref[span, :] = mix_ref[span, :] * factor + jnp.dot(
                    rounded, v, preferred_element_type=jnp.float32
                )
                top_ref[span, :] = top

    if last:
        for j in range(8):
            span = slice(j * 128, (j + 1) * 128)
            total = jnp.sum(sum_ref[span, :], axis=1, keepdims=True)
            out_ref[0:128, j * HD : (j + 1) * HD] = (mix_ref[span, :] / total).astype(jnp.bfloat16)
        total = got(key_refs[0], rider) + got(key_refs[1], rider) + energy_ref[...]
        put_wide(out_ref, total)
        out_ref[128:BLOCK, 512:1024] = jnp.zeros((16, 512), jnp.bfloat16)


def finish_kernel(first_ref, second_ref, attention_ref, captured_ref, share_ref):
    odd = place()[2]
    for swap in range(2):

        @pl.when(odd == swap)
        def _(swap=swap):
            for t, ref in enumerate((first_ref, second_ref)):
                head = t ^ swap
                attention_ref[:, head * 1024 : (head + 1) * 1024] = ref[0:128, :]

    received = [got_wide(first_ref), got_wide(second_ref)]
    row = lax.broadcasted_iota(jnp.int32, (RIDER, 128), 0)
    lane = lax.broadcasted_iota(jnp.int32, (RIDER, 128), 1)
    rows = lax.broadcasted_iota(jnp.int32, (2, 2), 0)
    columns = lax.broadcasted_iota(jnp.int32, (2, 2), 1)
    own, everything = {}, [0.0, 0.0]
    for g in range(2):
        sums = jnp.where(odd == g, received[0], received[1])
        for kind in range(2):
            n = 2 * g + kind
            captured_ref[n] = sums[:, n * RANK : (n + 1) * RANK] * (1.0 / TOKENS)
            here = lane == 64 * (1 - g)
            own[n] = jnp.sum(jnp.where(here & (row == kind), sums, 0.0))
            everything[kind] += 0.5 * jnp.sum(jnp.where(here & (row == kind + 2), sums, 0.0))
    share = jnp.zeros((2, 2), jnp.float32)
    for g in range(2):
        for kind in range(2):
            value = jnp.full((2, 2), KVH * own[2 * g + kind], jnp.float32) / everything[kind]
            share = jnp.where((rows == g) & (columns == kind), value, share)
    share_ref[...] = share


def vmem():
    return pl.BlockSpec(memory_space=pltpu.VMEM)


def rows(count):
    return jax.ShapeDtypeStruct((count, 256), jnp.bfloat16)


def small(kernel, out_shape, *inputs):
    return pl.pallas_call(
        kernel,
        out_shape=out_shape,
        in_specs=[vmem()] * len(inputs),
        out_specs=[vmem()] * len(out_shape),
        compiler_params=pltpu.CompilerParams(vmem_limit_bytes=6 * 1024 * 1024),
        cost_estimate=pl.CostEstimate(flops=1 << 20, bytes_accessed=1 << 18, transcendentals=0),
    )(*inputs)


def attend(q, arrays, units, state, tile=None, rider=None, energy=None):
    first, last = state is None, tile is not None
    wide = (2048, 128)
    carry = [
        jax.ShapeDtypeStruct(wide, jnp.bfloat16),
        jax.ShapeDtypeStruct((32, 128), jnp.float32),
        jax.ShapeDtypeStruct(wide, jnp.float32),
        jax.ShapeDtypeStruct(wide, jnp.float32),
        jax.ShapeDtypeStruct(wide, jnp.float32),
    ]
    tiles = (tile,) if last else (0, 1)
    keys = sum(128 * len(piece[4]) for unit in units for piece in unit)
    work = len(tiles) * 1024 * keys
    inputs = (list(q) if first else []) + list(arrays)
    aliases = {}
    if not first:
        if not last:
            aliases = {len(inputs) + n: n for n in range(5)}
        inputs += list(state)
    if last:
        inputs.append(energy)
        out_shape = [jax.ShapeDtypeStruct((BLOCK, 1024), jnp.bfloat16)]
        scratch = [pltpu.VMEM((1024, 128), jnp.float32)] * 3
    else:
        out_shape, scratch = carry, []
    return list(
        pl.pallas_call(
            functools.partial(attend_kernel, len(arrays), units, tiles, first, last, rider),
            out_shape=out_shape,
            in_specs=[vmem()] * len(inputs),
            out_specs=[vmem()] * len(out_shape),
            scratch_shapes=scratch,
            input_output_aliases=aliases,
            compiler_params=pltpu.CompilerParams(vmem_limit_bytes=20 * 1024 * 1024),
            cost_estimate=pl.CostEstimate(
                flops=4 * work * HD, bytes_accessed=1 << 20, transcendentals=work
            ),
            name="attend_last" if last else "attend",
        )(*inputs)
    )


def body(queries, keys, values, segments, basis):
    odd = lax.axis_index("y") & 1
    send0, send1, latents, energy = pl.pallas_call(
        prepare_kernel,
        out_shape=[
            rows(BLOCK + RIDER),
            rows(BLOCK + RIDER),
            jax.ShapeDtypeStruct((128, 128), jnp.bfloat16),
            jax.ShapeDtypeStruct((8, 128), jnp.float32),
        ],
        in_specs=[pl.BlockSpec(memory_space=pltpu.HBM)] * 4,
        out_specs=[vmem()] * 4,
        scratch_shapes=[
            pltpu.VMEM((128, 256), jnp.bfloat16),
            pltpu.VMEM((128, 256), jnp.bfloat16),
            pltpu.VMEM((1, 128), jnp.int32),
            pltpu.VMEM((2, 2, RANK, HD), jnp.bfloat16),
            pltpu.SemaphoreType.DMA((4,)),
        ],
        compiler_params=pltpu.CompilerParams(vmem_limit_bytes=66100000),
        name="prepare",
    )(keys, values, segments.reshape(1, 128), jnp.swapaxes(basis, 2, 3))
    kv = []
    for t, array in enumerate((send0, send1)):
        kv.append(lax.ppermute(array, COLUMN, to_heads(t)))
    slices = [lax.dynamic_slice_in_dim(queries, (odd ^ t) * 1024, 1024, 1) for t in range(2)]
    q = [lax.ppermute(slices[t], COLUMN, to_heads(t)) for t in range(2)]
    energy = added(energy, "c", 1)
    energy = added(energy, "xl", 1)

    def partner(array):
        return lax.ppermute(array, "c", [(0, 1), (1, 0)])

    def after(state, *arrays):
        state[2], *arrays = lax.optimization_barrier((state[2], *arrays))
        return arrays

    def piece(array, row, distance, other):
        return (array, row, distance, other, (None,) if distance == 9 else (0, 1))

    message = rows(HALF + RIDER)
    (own,) = small(start_kernel, [message], *kv, energy)
    eight = shifted(own, 8)
    up, down, both = small(
        once_kernel, [rows(HALF + RIDER + BLOCK), message, rows(2 * HALF)], own, eight
    )
    one, seven = shifted(up, 1), shifted(down, -1)
    other_zero_eight = partner(both)

    onward, both = small(split_kernel, [message, rows(2 * HALF + BLOCK)], one, seven)
    two, six = shifted(onward, 1), shifted(seven, -1)
    other_one_seven = partner(both)
    own, onward = lax.optimization_barrier((own, onward))
    state = attend(q, [own, eight], ((piece(0, 0, 0, False), piece(1, 0, 8, False)),), None)
    state = attend(
        None,
        [one, seven, other_zero_eight],
        (
            (piece(0, 0, 1, False), piece(1, 0, 7, False)),
            (piece(2, 0, 0, True), piece(2, HALF, 8, True)),
        ),
        state,
    )

    two, six = after(state, two, six)
    three, five = shifted(two, 1), shifted(six, -1)
    (both,) = small(pair_kernel, [rows(2 * HALF)], two, six)
    other_two_six = partner(both)
    state = attend(
        None,
        [two, six, other_one_seven],
        (
            (piece(0, 0, 2, False), piece(1, 0, 6, False)),
            (piece(2, 0, 1, True), piece(2, HALF, 7, True)),
        ),
        state,
    )

    three, five = after(state, three, five)
    four = shifted(three, 1)
    (both,) = small(pair_kernel, [rows(2 * HALF)], three, five)
    other_three_five = partner(both)
    state = attend(
        None,
        [three, five, other_two_six],
        (
            (piece(0, 0, 3, False), piece(1, 0, 5, False)),
            (piece(2, 0, 2, True), piece(2, HALF, 6, True)),
        ),
        state,
    )

    (four,) = after(state, four)
    four, energy = small(
        total_kernel,
        [message, jax.ShapeDtypeStruct((RIDER, 128), jnp.float32)],
        four,
        up,
        one,
        seven,
        two,
        six,
        three,
        five,
    )
    other_four = partner(four)
    energy = lax.ppermute(energy, "y", [(i, i ^ 2) for i in range(4)])
    state = attend(
        None,
        [four, one, other_one_seven, other_three_five],
        (
            (
                piece(0, 0, 4, False),
                piece(1, HALF + RIDER, 9, False),
                piece(2, 2 * HALF, 9, True),
            ),
            (piece(3, 0, 3, True), piece(3, HALF, 5, True)),
        ),
        state,
    )
    units = ((piece(0, 0, 4, True),),)
    back = []
    for t in range(2):
        (mixed,) = attend(
            None, [other_four, four], units, state, t, HALF, energy
        )
        back.append(lax.ppermute(mixed, COLUMN, [(d, s) for s, d in to_heads(t)]))
    attention, captured, share = small(
        finish_kernel,
        [
            jax.ShapeDtypeStruct((128, 2048), jnp.bfloat16),
            jax.ShapeDtypeStruct((4, RANK, RANK), jnp.float32),
            jax.ShapeDtypeStruct((2, 2), jnp.float32),
        ],
        *back,
    )
    return (attention, latents, captured.reshape(2, 2, RANK, RANK), share)


def solution(mesh):
    torus = Mesh(mesh.devices.reshape(2, 8, 4, 2, 2), ("a", "z", "y", "xl", "c"))
    in_specs = (P(SEQ, KV), P(SEQ, KV), P(SEQ, KV), P(SEQ), P(KV, None, None, None))
    out_specs = (P(SEQ, KV), P(SEQ, KV), P(KV, None, None, None), P(KV, None))

    return jax.shard_map(body, mesh=torus, in_specs=in_specs, out_specs=out_specs, check_vma=False)
```

```python
import functools
import math

import jax
import jax.numpy as jnp
from jax import lax
from jax.experimental import pallas as pl
from jax.experimental.pallas import tpu as pltpu
from jax.sharding import Mesh
from jax.sharding import PartitionSpec as P

HD = 128
KVH = 8
RANK = 32
TOKENS = 8192
SLABS = 16
SEQ = ("a", "z", "y")
KV = ("xl", "c")
RING = ("a", "z")
COLUMN = ("y", "c")
BLOCK = 144
HALF = 2 * BLOCK
RIDER = 32
SCALE2 = HD**-0.5 * math.log2(math.e)
FIRST = -1e30
MASKED = -2e30
FAR = 1e9


def to_heads(t):
    pairs = []
    for y in range(4):
        for c in range(2):
            head = (y & 1) ^ t
            pairs.append((y * 2 + c, (2 * c + head) * 2 + (y >> 1)))
    return pairs


def shifted(array, by):
    return lax.ppermute(array, RING, [(i, (i + by) % SLABS) for i in range(SLABS)])


def added(array, axis, distance):
    size = lax.axis_size(axis)
    return array + lax.ppermute(array, axis, [(i, i ^ distance) for i in range(size)])


def place():
    slab = lax.axis_index("a") * 8 + lax.axis_index("z")
    return slab, lax.axis_index("c"), lax.axis_index("y") & 1


def encoded(total):
    high = total.astype(jnp.bfloat16)
    rest = (total - high.astype(jnp.float32)).astype(jnp.bfloat16)
    return high, rest


def put(ref, row, total):
    ref[row : row + RIDER, 0:128], ref[row : row + RIDER, 128:256] = encoded(total)


def got(ref, row):
    rows = slice(row, row + RIDER)
    return ref[rows, 0:128].astype(jnp.float32) + ref[rows, 128:256].astype(jnp.float32)


def put_wide(ref, total):
    for n, part in enumerate(encoded(total)):
        for m in range(2):
            lanes = slice(m * 256 + n * 128, m * 256 + n * 128 + 128)
            ref[128:BLOCK, lanes] = part[m * 16 : (m + 1) * 16, :]


def got_wide(ref):
    rows = []
    for m in range(2):
        high = ref[128:BLOCK, m * 256 : m * 256 + 128].astype(jnp.float32)
        rest = ref[128:BLOCK, m * 256 + 128 : m * 256 + 256].astype(jnp.float32)
        rows.append(high + rest)
    return jnp.concatenate(rows, axis=0)


def prepare_kernel(
    keys_hbm,
    values_hbm,
    segments_hbm,
    basis_hbm,
    first_ref,
    second_ref,
    latents_ref,
    energy_ref,
    keys_ref,
    values_ref,
    segments_ref,
    basis_ref,
    semaphores,
):
    loads = [
        pltpu.make_async_copy(source, target, semaphores.at[n])
        for n, (source, target) in enumerate(
            (
                (segments_hbm, segments_ref),
                (keys_hbm, keys_ref),
                (values_hbm, values_ref),
                (basis_hbm, basis_ref),
            )
        )
    ]
    for copy in loads:
        copy.start()
    for copy in loads:
        copy.wait()
    ids = segments_ref[...]
    n1 = jnp.sum((ids < 1).astype(jnp.float32))
    n2 = jnp.sum((ids < 2).astype(jnp.float32))
    lanes = lax.broadcasted_iota(jnp.int32, (16, 256), 1)
    counts = jnp.where(lanes < 128, n1, n2).astype(jnp.bfloat16)
    projected, energies = [], []
    for g in range(2):
        for kind, ref in enumerate((keys_ref, values_ref)):
            rows = ref[:, g * HD : (g + 1) * HD]
            projected.append(
                lax.dot_general(
                    rows,
                    basis_ref[g, kind],
                    (((1,), (1,)), ((), ())),
                    preferred_element_type=jnp.float32,
                )
            )
            squares = rows.astype(jnp.float32)
            energies.append(jnp.sum(squares * squares))
    latents = jnp.concatenate(projected, axis=1)
    latents_ref[...] = latents.astype(jnp.bfloat16)
    seen = lax.dot_general(
        latents,
        latents,
        (((0,), (0,)), ((), ())),
        precision=lax.Precision.HIGHEST,
        preferred_element_type=jnp.float32,
    )
    lane = lax.broadcasted_iota(jnp.int32, (RIDER, 128), 1) // RANK
    row = lax.broadcasted_iota(jnp.int32, (RIDER, 128), 0)
    riders = []
    for g in range(2):
        other = jnp.where(row == 0, energies[2 * g], jnp.where(row == 1, energies[2 * g + 1], 0.0))
        for n in (2 * g, 2 * g + 1):
            other = jnp.where(lane == n, seen[n * RANK : (n + 1) * RANK, :], other)
        riders.append(other)
    row8 = lax.broadcasted_iota(jnp.int32, (8, 128), 0)
    energy_ref[...] = jnp.where(
        row8 == 0,
        energies[0] + energies[2],
        jnp.where(row8 == 1, energies[1] + energies[3], 0.0),
    )
    for odd in range(2):

        @pl.when(place()[2] == odd)
        def _(odd=odd):
            for ref, head in ((first_ref, odd), (second_ref, 1 - odd)):
                ref[0:128, 0:HD] = keys_ref[:, head * HD : (head + 1) * HD]
                ref[0:128, HD : 2 * HD] = values_ref[:, head * HD : (head + 1) * HD]
                put(ref, BLOCK, riders[head])

    for ref in (first_ref, second_ref):
        ref[128:BLOCK, :] = counts


def start_kernel(first_ref, second_ref, energy_ref, out_ref):
    out_ref[0:BLOCK, :] = first_ref[0:BLOCK, :]
    out_ref[BLOCK:HALF, :] = second_ref[0:BLOCK, :]
    lane = lax.broadcasted_iota(jnp.int32, (RIDER, 128), 1) // 64
    row = lax.broadcasted_iota(jnp.int32, (RIDER, 128), 0)
    energy = jnp.where(
        row == 2, energy_ref[0:1, :], jnp.where(row == 3, energy_ref[1:2, :], 0.0)
    )
    energy = jnp.where(lane == 1 - place()[2], energy, 0.0)
    put(out_ref, HALF, got(first_ref, BLOCK) + got(second_ref, BLOCK) + energy)


def once_kernel(own_ref, eight_ref, up_ref, down_ref, both_ref):
    both = got(own_ref, HALF) + got(eight_ref, HALF)
    up_ref[0:HALF, :] = own_ref[0:HALF, :]
    down_ref[0:HALF, :] = eight_ref[0:HALF, :]
    put(up_ref, HALF, both)
    put(down_ref, HALF, both)
    for odd in range(2):

        @pl.when(place()[2] == odd)
        def _(odd=odd):
            row = (1 - odd) * BLOCK
            up_ref[HALF + RIDER : HALF + RIDER + BLOCK, :] = eight_ref[row : row + BLOCK, :]

    both_ref[0:HALF, :] = own_ref[0:HALF, :]
    both_ref[HALF : 2 * HALF, :] = eight_ref[0:HALF, :]


def split_kernel(one_ref, seven_ref, next_ref, both_ref):
    next_ref[...] = one_ref[0 : HALF + RIDER, :]
    both_ref[0:HALF, :] = one_ref[0:HALF, :]
    both_ref[HALF : 2 * HALF, :] = seven_ref[0:HALF, :]
    both_ref[2 * HALF : 2 * HALF + BLOCK, :] = one_ref[HALF + RIDER : HALF + RIDER + BLOCK, :]


def pair_kernel(first_ref, second_ref, both_ref):
    both_ref[0:HALF, :] = first_ref[0:HALF, :]
    both_ref[HALF : 2 * HALF, :] = second_ref[0:HALF, :]


def total_kernel(*refs):
    *terms, out_ref, energy_ref = refs
    out_ref[0:HALF, :] = terms[0][0:HALF, :]
    total = functools.reduce(jnp.add, [got(ref, HALF) for ref in terms])
    put(out_ref, HALF, total)
    lane = lax.broadcasted_iota(jnp.int32, (RIDER, 128), 1) // 64
    row = lax.broadcasted_iota(jnp.int32, (RIDER, 128), 0)
    energies = (lane == 1 - place()[2]) & ((row == 2) | (row == 3))
    energy_ref[...] = jnp.where(energies, 2.0 * total, 0.0)


def attend_kernel(count, units, tiles, first, last, rider, *refs):
    refs = list(refs)
    if first:
        q_in = [refs.pop(0) for _ in range(2)]
    key_refs = [refs.pop(0) for _ in range(count)]
    state_in = None if first else [refs.pop(0) for _ in range(5)]
    if last:
        energy_ref = refs.pop(0)
        out_ref = refs.pop(0)
        q_ref = state_in[0]
        top_ref, sum_ref, mix_ref = refs
    else:
        q_ref, starts_ref, top_ref, sum_ref, mix_ref = refs
    slab, core, odd = place()
    origin = tiles[0] * 1024 if last else 0

    found_units = []
    for unit in units:
        found = []
        for array, row, distance, partner, rounds in unit:
            base = ((slab - distance) & (SLABS - 1)) * 512 + (1 - core if partner else core) * 256
            for n, t in enumerate(rounds):
                block = base + (128 if t is None else (odd ^ t) * 128)
                found.append((key_refs[array], row + n * BLOCK, block))
        found_units.append(found)

    one = jnp.full((16, 128), FAR, jnp.float32) if first else state_in[1][0:16, :]
    two = jnp.full((16, 128), FAR, jnp.float32) if first else state_in[1][16:32, :]
    for found in found_units:
        for ref, row, base in found:
            counts = ref[row + 128 : row + BLOCK, :].astype(jnp.float32)
            at = base.astype(jnp.float32)
            n1, n2 = counts[:, :128], counts[:, 128:]
            one = jnp.minimum(one, jnp.where(n1 < 128.0, at + n1, FAR))
            two = jnp.minimum(two, jnp.where(n2 < 128.0, at + n2, FAR))
    if not last:
        starts_ref[0:16, :] = one
        starts_ref[16:32, :] = two
    start1 = jnp.min(one).astype(jnp.int32)
    start2 = jnp.min(two).astype(jnp.int32)

    if first:
        for t in range(2):
            for j in range(8):
                q_ref[t * 1024 + j * 128 : t * 1024 + (j + 1) * 128, :] = q_in[t][
                    0:128, j * HD : (j + 1) * HD
                ]
        top_ref[...] = jnp.full(top_ref.shape, FIRST, jnp.float32)
        sum_ref[...] = jnp.zeros(sum_ref.shape, jnp.float32)
        mix_ref[...] = jnp.zeros(mix_ref.shape, jnp.float32)
    elif last:
        span = slice(origin, origin + 1024)
        top_ref[...] = state_in[2][span, :]
        sum_ref[...] = state_in[3][span, :]
        mix_ref[...] = state_in[4][span, :]

    row_iota = lax.broadcasted_iota(jnp.int32, (128, 128), 0)
    lane_iota = lax.broadcasted_iota(jnp.int32, (128, 128), 1)

    def low_of(position):
        return jnp.where(position >= start2, start2, jnp.where(position >= start1, start1, 0))

    q_base = {t: slab * 512 + core * 256 + (odd ^ t) * 128 for t in tiles}
    for found in found_units:
        needed = functools.reduce(
            jnp.logical_or,
            [
                (base <= q_base[t]) & (base + 127 >= low_of(q_base[t]))
                for t in tiles
                for ref, row, base in found
            ],
        )

        @pl.when(needed)
        def _(found=found):
            k = jnp.concatenate([r[row : row + 128, 0:HD] for r, row, _ in found], axis=0)
            v = jnp.concatenate([r[row : row + 128, HD : 2 * HD] for r, row, _ in found], axis=0)
            scores = {
                t: lax.dot_general(
                    q_ref[t * 1024 : (t + 1) * 1024, :],
                    k,
                    (((1,), (1,)), ((), ())),
                    preferred_element_type=jnp.float32,
                )
                for t in tiles
            }
            for t in tiles:
                q_pos = q_base[t] + row_iota
                lows = low_of(q_pos)
                parts = []
                for n, (ref, row, base) in enumerate(found):
                    k_pos = base + lane_iota
                    mask = (k_pos >= lows) & (k_pos <= q_pos)
                    mask = jnp.concatenate([mask] * 8, axis=0)
                    parts.append(
                        jnp.where(mask, scores[t][:, n * 128 : (n + 1) * 128], MASKED)
                    )
                best = functools.reduce(jnp.maximum, parts)
                span = slice(t * 1024 - origin, (t + 1) * 1024 - origin)
                top_old = top_ref[span, :]
                top = jnp.maximum(top_old, jnp.max(best, axis=1, keepdims=True))
                factor = jnp.exp2((top_old - top) * SCALE2)
                weights = [jnp.exp2((part - top) * SCALE2) for part in parts]
                sum_ref[span, :] = sum_ref[span, :] * factor + functools.reduce(jnp.add, weights)
                rounded = jnp.concatenate([w.astype(jnp.bfloat16) for w in weights], axis=1)
                mix_ref[span, :] = mix_ref[span, :] * factor + jnp.dot(
                    rounded, v, preferred_element_type=jnp.float32
                )
                top_ref[span, :] = top

    if last:
        for j in range(8):
            span = slice(j * 128, (j + 1) * 128)
            total = jnp.sum(sum_ref[span, :], axis=1, keepdims=True)
            out_ref[0:128, j * HD : (j + 1) * HD] = (mix_ref[span, :] / total).astype(jnp.bfloat16)
        total = got(key_refs[0], rider) + got(key_refs[1], rider) + energy_ref[...]
        put_wide(out_ref, total)
        out_ref[128:BLOCK, 512:1024] = jnp.zeros((16, 512), jnp.bfloat16)


def finish_kernel(first_ref, second_ref, attention_ref, captured_ref, share_ref):
    odd = place()[2]
    for swap in range(2):

        @pl.when(odd == swap)
        def _(swap=swap):
            for t, ref in enumerate((first_ref, second_ref)):
                head = t ^ swap
                attention_ref[:, head * 1024 : (head + 1) * 1024] = ref[0:128, :]

    received = [got_wide(first_ref), got_wide(second_ref)]
    row = lax.broadcasted_iota(jnp.int32, (RIDER, 128), 0)
    lane = lax.broadcasted_iota(jnp.int32, (RIDER, 128), 1)
    rows = lax.broadcasted_iota(jnp.int32, (2, 2), 0)
    columns = lax.broadcasted_iota(jnp.int32, (2, 2), 1)
    own, everything = {}, [0.0, 0.0]
    for g in range(2):
        sums = jnp.where(odd == g, received[0], received[1])
        for kind in range(2):
            n = 2 * g + kind
            captured_ref[n] = sums[:, n * RANK : (n + 1) * RANK] * (1.0 / TOKENS)
            here = lane == 64 * (1 - g)
            own[n] = jnp.sum(jnp.where(here & (row == kind), sums, 0.0))
            everything[kind] += 0.5 * jnp.sum(jnp.where(here & (row == kind + 2), sums, 0.0))
    share = jnp.zeros((2, 2), jnp.float32)
    for g in range(2):
        for kind in range(2):
            value = jnp.full((2, 2), KVH * own[2 * g + kind], jnp.float32) / everything[kind]
            share = jnp.where((rows == g) & (columns == kind), value, share)
    share_ref[...] = share


def vmem():
    return pl.BlockSpec(memory_space=pltpu.VMEM)


def rows(count):
    return jax.ShapeDtypeStruct((count, 256), jnp.bfloat16)


def small(kernel, out_shape, *inputs):
    return pl.pallas_call(
        kernel,
        out_shape=out_shape,
        in_specs=[vmem()] * len(inputs),
        out_specs=[vmem()] * len(out_shape),
        compiler_params=pltpu.CompilerParams(vmem_limit_bytes=6 * 1024 * 1024),
        cost_estimate=pl.CostEstimate(flops=1 << 20, bytes_accessed=1 << 18, transcendentals=0),
    )(*inputs)


def attend(q, arrays, units, state, tile=None, rider=None, energy=None):
    first, last = state is None, tile is not None
    wide = (2048, 128)
    carry = [
        jax.ShapeDtypeStruct(wide, jnp.bfloat16),
        jax.ShapeDtypeStruct((32, 128), jnp.float32),
        jax.ShapeDtypeStruct(wide, jnp.float32),
        jax.ShapeDtypeStruct(wide, jnp.float32),
        jax.ShapeDtypeStruct(wide, jnp.float32),
    ]
    tiles = (tile,) if last else (0, 1)
    keys = sum(128 * len(piece[4]) for unit in units for piece in unit)
    work = len(tiles) * 1024 * keys
    inputs = (list(q) if first else []) + list(arrays)
    aliases = {}
    if not first:
        if not last:
            aliases = {len(inputs) + n: n for n in range(5)}
        inputs += list(state)
    if last:
        inputs.append(energy)
        out_shape = [jax.ShapeDtypeStruct((BLOCK, 1024), jnp.bfloat16)]
        scratch = [pltpu.VMEM((1024, 128), jnp.float32)] * 3
    else:
        out_shape, scratch = carry, []
    return list(
        pl.pallas_call(
            functools.partial(attend_kernel, len(arrays), units, tiles, first, last, rider),
            out_shape=out_shape,
            in_specs=[vmem()] * len(inputs),
            out_specs=[vmem()] * len(out_shape),
            scratch_shapes=scratch,
            input_output_aliases=aliases,
            compiler_params=pltpu.CompilerParams(vmem_limit_bytes=20 * 1024 * 1024),
            cost_estimate=pl.CostEstimate(
                flops=4 * work * HD, bytes_accessed=1 << 20, transcendentals=work
            ),
            name="attend_last" if last else "attend",
        )(*inputs)
    )


def body(queries, keys, values, segments, basis):
    odd = lax.axis_index("y") & 1
    send0, send1, latents, energy = pl.pallas_call(
        prepare_kernel,
        out_shape=[
            rows(BLOCK + RIDER),
            rows(BLOCK + RIDER),
            jax.ShapeDtypeStruct((128, 128), jnp.bfloat16),
            jax.ShapeDtypeStruct((8, 128), jnp.float32),
        ],
        in_specs=[pl.BlockSpec(memory_space=pltpu.HBM)] * 4,
        out_specs=[vmem()] * 4,
        scratch_shapes=[
            pltpu.VMEM((128, 256), jnp.bfloat16),
            pltpu.VMEM((128, 256), jnp.bfloat16),
            pltpu.VMEM((1, 128), jnp.int32),
            pltpu.VMEM((2, 2, RANK, HD), jnp.bfloat16),
            pltpu.SemaphoreType.DMA((4,)),
        ],
        compiler_params=pltpu.CompilerParams(vmem_limit_bytes=66100000),
        name="prepare",
    )(keys, values, segments.reshape(1, 128), jnp.swapaxes(basis, 2, 3))
    kv = []
    for t, array in enumerate((send0, send1)):
        kv.append(lax.ppermute(array, COLUMN, to_heads(t)))
    slices = [lax.dynamic_slice_in_dim(queries, (odd ^ t) * 1024, 1024, 1) for t in range(2)]
    q = [lax.ppermute(slices[t], COLUMN, to_heads(t)) for t in range(2)]
    energy = added(energy, "c", 1)
    energy = added(energy, "xl", 1)

    def partner(array):
        return lax.ppermute(array, "c", [(0, 1), (1, 0)])

    def after(state, *arrays):
        state[2], *arrays = lax.optimization_barrier((state[2], *arrays))
        return arrays

    def piece(array, row, distance, other):
        return (array, row, distance, other, (None,) if distance == 9 else (0, 1))

    message = rows(HALF + RIDER)
    (own,) = small(start_kernel, [message], *kv, energy)
    eight = shifted(own, 8)
    up, down, both = small(
        once_kernel, [rows(HALF + RIDER + BLOCK), message, rows(2 * HALF)], own, eight
    )
    one, seven = shifted(up, 1), shifted(down, -1)
    other_zero_eight = partner(both)

    onward, both = small(split_kernel, [message, rows(2 * HALF + BLOCK)], one, seven)
    two, six = shifted(onward, 1), shifted(seven, -1)
    other_one_seven = partner(both)
    own, onward = lax.optimization_barrier((own, onward))
    state = attend(q, [own, eight], ((piece(0, 0, 0, False), piece(1, 0, 8, False)),), None)
    state = attend(
        None,
        [one, seven, other_zero_eight],
        (
            (piece(0, 0, 1, False), piece(1, 0, 7, False)),
            (piece(2, 0, 0, True), piece(2, HALF, 8, True)),
        ),
        state,
    )

    two, six = after(state, two, six)
    three, five = shifted(two, 1), shifted(six, -1)
    (both,) = small(pair_kernel, [rows(2 * HALF)], two, six)
    other_two_six = partner(both)
    state = attend(
        None,
        [two, six, other_one_seven],
        (
            (piece(0, 0, 2, False), piece(1, 0, 6, False)),
            (piece(2, 0, 1, True), piece(2, HALF, 7, True)),
        ),
        state,
    )
    state = attend(None, [other_two_six], ((piece(0, 0, 2, True), piece(0, HALF, 6, True)),), state)

    three, five = after(state, three, five)
    four = shifted(three, 1)
    (both,) = small(pair_kernel, [rows(2 * HALF)], three, five)
    other_three_five = partner(both)
    state = attend(None, [three, five], ((piece(0, 0, 3, False), piece(1, 0, 5, False)),), state)

    (four,) = after(state, four)
    four, energy = small(
        total_kernel,
        [message, jax.ShapeDtypeStruct((RIDER, 128), jnp.float32)],
        four,
        up,
        one,
        seven,
        two,
        six,
        three,
        five,
    )
    other_four = partner(four)
    energy = lax.ppermute(energy, "y", [(i, i ^ 2) for i in range(4)])
    state = attend(
        None, [other_three_five], ((piece(0, 0, 3, True), piece(0, HALF, 5, True)),), state
    )
    units = (
        (
            piece(1, 0, 4, False),
            piece(2, HALF + RIDER, 9, False),
            piece(3, 2 * HALF, 9, True),
        ),
        (piece(0, 0, 4, True),),
    )
    arrays = [other_four, four, one, other_one_seven]
    back = []
    for t in range(2):
        (mixed,) = attend(
            None, arrays, units, state, t, HALF, energy
        )
        back.append(lax.ppermute(mixed, COLUMN, [(d, s) for s, d in to_heads(t)]))
    attention, captured, share = small(
        finish_kernel,
        [
            jax.ShapeDtypeStruct((128, 2048), jnp.bfloat16),
            jax.ShapeDtypeStruct((4, RANK, RANK), jnp.float32),
            jax.ShapeDtypeStruct((2, 2), jnp.float32),
        ],
        *back,
    )
    return (attention, latents, captured.reshape(2, 2, RANK, RANK), share)


def solution(mesh):
    torus = Mesh(mesh.devices.reshape(2, 8, 4, 2, 2), ("a", "z", "y", "xl", "c"))
    in_specs = (P(SEQ, KV), P(SEQ, KV), P(SEQ, KV), P(SEQ), P(KV, None, None, None))
    out_specs = (P(SEQ, KV), P(SEQ, KV), P(KV, None, None, None), P(KV, None))

    return jax.shard_map(body, mesh=torus, in_specs=in_specs, out_specs=out_specs, check_vma=False)
```

```python
import functools
import math

import jax
import jax.numpy as jnp
from jax import lax
from jax.experimental import pallas as pl
from jax.experimental.pallas import tpu as pltpu
from jax.sharding import Mesh
from jax.sharding import PartitionSpec as P

HD = 128
KVH = 8
RANK = 32
TOKENS = 8192
SLABS = 16
SEQ = ("a", "z", "y")
KV = ("xl", "c")
RING = ("a", "z")
COLUMN = ("y", "c")
BLOCK = 144
HALF = 2 * BLOCK
RIDER = 32
SCALE2 = HD**-0.5 * math.log2(math.e)
FIRST = -1e30
MASKED = -2e30
FAR = 1e9


def to_heads(t):
    pairs = []
    for y in range(4):
        for c in range(2):
            head = (y & 1) ^ t
            pairs.append((y * 2 + c, (2 * c + head) * 2 + (y >> 1)))
    return pairs


def shifted(array, by):
    return lax.ppermute(array, RING, [(i, (i + by) % SLABS) for i in range(SLABS)])


def added(array, axis, distance):
    size = lax.axis_size(axis)
    return array + lax.ppermute(array, axis, [(i, i ^ distance) for i in range(size)])


def place():
    slab = lax.axis_index("a") * 8 + lax.axis_index("z")
    return slab, lax.axis_index("c"), lax.axis_index("y") & 1


def encoded(total):
    high = total.astype(jnp.bfloat16)
    rest = (total - high.astype(jnp.float32)).astype(jnp.bfloat16)
    return high, rest


def put(ref, row, total):
    ref[row : row + RIDER, 0:128], ref[row : row + RIDER, 128:256] = encoded(total)


def got(ref, row):
    rows = slice(row, row + RIDER)
    return ref[rows, 0:128].astype(jnp.float32) + ref[rows, 128:256].astype(jnp.float32)


def put_wide(ref, total):
    for n, part in enumerate(encoded(total)):
        for m in range(2):
            lanes = slice(m * 256 + n * 128, m * 256 + n * 128 + 128)
            ref[128:BLOCK, lanes] = part[m * 16 : (m + 1) * 16, :]


def got_wide(ref):
    rows = []
    for m in range(2):
        high = ref[128:BLOCK, m * 256 : m * 256 + 128].astype(jnp.float32)
        rest = ref[128:BLOCK, m * 256 + 128 : m * 256 + 256].astype(jnp.float32)
        rows.append(high + rest)
    return jnp.concatenate(rows, axis=0)


def prepare_kernel(
    keys_hbm,
    values_hbm,
    segments_hbm,
    basis_hbm,
    first_ref,
    second_ref,
    latents_ref,
    energy_ref,
    keys_ref,
    values_ref,
    segments_ref,
    basis_ref,
    semaphores,
):
    loads = [
        pltpu.make_async_copy(source, target, semaphores.at[n])
        for n, (source, target) in enumerate(
            (
                (segments_hbm, segments_ref),
                (keys_hbm, keys_ref),
                (values_hbm, values_ref),
                (basis_hbm, basis_ref),
            )
        )
    ]
    for copy in loads:
        copy.start()
    for copy in loads:
        copy.wait()
    ids = segments_ref[...]
    n1 = jnp.sum((ids < 1).astype(jnp.float32))
    n2 = jnp.sum((ids < 2).astype(jnp.float32))
    lanes = lax.broadcasted_iota(jnp.int32, (16, 256), 1)
    counts = jnp.where(lanes < 128, n1, n2).astype(jnp.bfloat16)
    projected, energies = [], []
    for g in range(2):
        for kind, ref in enumerate((keys_ref, values_ref)):
            rows = ref[:, g * HD : (g + 1) * HD]
            projected.append(
                lax.dot_general(
                    rows,
                    basis_ref[g, kind],
                    (((1,), (1,)), ((), ())),
                    preferred_element_type=jnp.float32,
                )
            )
            squares = rows.astype(jnp.float32)
            energies.append(jnp.sum(squares * squares))
    latents = jnp.concatenate(projected, axis=1)
    latents_ref[...] = latents.astype(jnp.bfloat16)
    seen = lax.dot_general(
        latents,
        latents,
        (((0,), (0,)), ((), ())),
        precision=lax.Precision.HIGHEST,
        preferred_element_type=jnp.float32,
    )
    lane = lax.broadcasted_iota(jnp.int32, (RIDER, 128), 1) // RANK
    row = lax.broadcasted_iota(jnp.int32, (RIDER, 128), 0)
    riders = []
    for g in range(2):
        other = jnp.where(row == 0, energies[2 * g], jnp.where(row == 1, energies[2 * g + 1], 0.0))
        for n in (2 * g, 2 * g + 1):
            other = jnp.where(lane == n, seen[n * RANK : (n + 1) * RANK, :], other)
        riders.append(other)
    row8 = lax.broadcasted_iota(jnp.int32, (8, 128), 0)
    energy_ref[...] = jnp.where(
        row8 == 0,
        energies[0] + energies[2],
        jnp.where(row8 == 1, energies[1] + energies[3], 0.0),
    )
    for odd in range(2):

        @pl.when(place()[2] == odd)
        def _(odd=odd):
            for ref, head in ((first_ref, odd), (second_ref, 1 - odd)):
                ref[0:128, 0:HD] = keys_ref[:, head * HD : (head + 1) * HD]
                ref[0:128, HD : 2 * HD] = values_ref[:, head * HD : (head + 1) * HD]
                put(ref, BLOCK, riders[head])

    for ref in (first_ref, second_ref):
        ref[128:BLOCK, :] = counts


def start_kernel(first_ref, second_ref, energy_ref, out_ref):
    out_ref[0:BLOCK, :] = first_ref[0:BLOCK, :]
    out_ref[BLOCK:HALF, :] = second_ref[0:BLOCK, :]
    lane = lax.broadcasted_iota(jnp.int32, (RIDER, 128), 1) // 64
    row = lax.broadcasted_iota(jnp.int32, (RIDER, 128), 0)
    energy = jnp.where(
        row == 2, energy_ref[0:1, :], jnp.where(row == 3, energy_ref[1:2, :], 0.0)
    )
    energy = jnp.where(lane == 1 - place()[2], energy, 0.0)
    put(out_ref, HALF, got(first_ref, BLOCK) + got(second_ref, BLOCK) + energy)


def once_kernel(own_ref, eight_ref, one_ref, up_ref, down_ref, three_ref):
    up_ref[0:HALF, :] = one_ref[0:HALF, :]
    down_ref[0:HALF, :] = eight_ref[0:HALF, :]
    put(up_ref, HALF, got(one_ref, HALF) + got(eight_ref, HALF))
    put(down_ref, HALF, got(own_ref, HALF) + got(eight_ref, HALF))
    for odd in range(2):

        @pl.when(place()[2] == odd)
        def _(odd=odd):
            row = (1 - odd) * BLOCK
            up_ref[HALF + RIDER : HALF + RIDER + BLOCK, :] = eight_ref[row : row + BLOCK, :]

    for n, ref in enumerate((own_ref, eight_ref, one_ref)):
        three_ref[n * HALF : (n + 1) * HALF, :] = ref[0:HALF, :]


def split_kernel(two_ref, seven_ref, next_ref, both_ref):
    next_ref[...] = two_ref[0 : HALF + RIDER, :]
    both_ref[0:HALF, :] = two_ref[0:HALF, :]
    both_ref[HALF : 2 * HALF, :] = seven_ref[0:HALF, :]
    both_ref[2 * HALF : 2 * HALF + BLOCK, :] = two_ref[HALF + RIDER : HALF + RIDER + BLOCK, :]


def pair_kernel(first_ref, second_ref, both_ref):
    both_ref[0:HALF, :] = first_ref[0:HALF, :]
    both_ref[HALF : 2 * HALF, :] = second_ref[0:HALF, :]


def total_kernel(four_ref, five_ref, own_ref, eight_ref, one_ref, *refs):
    two_ref, three_ref, seven_ref, six_ref, twelve_ref, out_ref, energy_ref = refs
    out_ref[0:HALF, :] = four_ref[0:HALF, :]
    out_ref[HALF + RIDER : 2 * HALF + RIDER, :] = five_ref[0:HALF, :]
    total = got(own_ref, HALF) + got(eight_ref, HALF) + got(one_ref, HALF)
    total += got(two_ref, HALF) + got(three_ref, HALF) + got(four_ref, HALF)
    total += got(seven_ref, HALF) + got(six_ref, HALF) + got(five_ref, HALF)
    total += got(twelve_ref, 0)
    put(out_ref, HALF, total)
    lane = lax.broadcasted_iota(jnp.int32, (RIDER, 128), 1) // 64
    row = lax.broadcasted_iota(jnp.int32, (RIDER, 128), 0)
    energies = (lane == 1 - place()[2]) & ((row == 2) | (row == 3))
    energy_ref[...] = jnp.where(energies, 2.0 * total, 0.0)


def attend_kernel(count, units, tiles, first, last, rider, *refs):
    refs = list(refs)
    if first:
        q_in = [refs.pop(0) for _ in range(2)]
    key_refs = [refs.pop(0) for _ in range(count)]
    state_in = None if first else [refs.pop(0) for _ in range(5)]
    if last:
        energy_ref = refs.pop(0)
        out_ref = refs.pop(0)
        q_ref = state_in[0]
        top_ref, sum_ref, mix_ref = refs
    else:
        q_ref, starts_ref, top_ref, sum_ref, mix_ref = refs
    slab, core, odd = place()
    origin = tiles[0] * 1024 if last else 0

    found_units = []
    for unit in units:
        found = []
        for array, row, distance, partner, rounds in unit:
            base = ((slab - distance) & (SLABS - 1)) * 512 + (1 - core if partner else core) * 256
            for n, t in enumerate(rounds):
                block = base + (128 if t is None else (odd ^ t) * 128)
                found.append((key_refs[array], row + n * BLOCK, block))
        found_units.append(found)

    one = jnp.full((16, 128), FAR, jnp.float32) if first else state_in[1][0:16, :]
    two = jnp.full((16, 128), FAR, jnp.float32) if first else state_in[1][16:32, :]
    for found in found_units:
        for ref, row, base in found:
            counts = ref[row + 128 : row + BLOCK, :].astype(jnp.float32)
            at = base.astype(jnp.float32)
            n1, n2 = counts[:, :128], counts[:, 128:]
            one = jnp.minimum(one, jnp.where(n1 < 128.0, at + n1, FAR))
            two = jnp.minimum(two, jnp.where(n2 < 128.0, at + n2, FAR))
    if not last:
        starts_ref[0:16, :] = one
        starts_ref[16:32, :] = two
    start1 = jnp.min(one).astype(jnp.int32)
    start2 = jnp.min(two).astype(jnp.int32)

    if first:
        for t in range(2):
            for j in range(8):
                q_ref[t * 1024 + j * 128 : t * 1024 + (j + 1) * 128, :] = q_in[t][
                    0:128, j * HD : (j + 1) * HD
                ]
        top_ref[...] = jnp.full(top_ref.shape, FIRST, jnp.float32)
        sum_ref[...] = jnp.zeros(sum_ref.shape, jnp.float32)
        mix_ref[...] = jnp.zeros(mix_ref.shape, jnp.float32)
    elif last:
        span = slice(origin, origin + 1024)
        top_ref[...] = state_in[2][span, :]
        sum_ref[...] = state_in[3][span, :]
        mix_ref[...] = state_in[4][span, :]

    row_iota = lax.broadcasted_iota(jnp.int32, (128, 128), 0)
    lane_iota = lax.broadcasted_iota(jnp.int32, (128, 128), 1)

    def low_of(position):
        return jnp.where(position >= start2, start2, jnp.where(position >= start1, start1, 0))

    q_base = {t: slab * 512 + core * 256 + (odd ^ t) * 128 for t in tiles}
    for found in found_units:
        needed = functools.reduce(
            jnp.logical_or,
            [
                (base <= q_base[t]) & (base + 127 >= low_of(q_base[t]))
                for t in tiles
                for ref, row, base in found
            ],
        )

        @pl.when(needed)
        def _(found=found):
            k = jnp.concatenate([r[row : row + 128, 0:HD] for r, row, _ in found], axis=0)
            v = jnp.concatenate([r[row : row + 128, HD : 2 * HD] for r, row, _ in found], axis=0)
            scores = {
                t: lax.dot_general(
                    q_ref[t * 1024 : (t + 1) * 1024, :],
                    k,
                    (((1,), (1,)), ((), ())),
                    preferred_element_type=jnp.float32,
                )
                for t in tiles
            }
            for t in tiles:
                q_pos = q_base[t] + row_iota
                lows = low_of(q_pos)
                parts = []
                for n, (ref, row, base) in enumerate(found):
                    k_pos = base + lane_iota
                    mask = (k_pos >= lows) & (k_pos <= q_pos)
                    mask = jnp.concatenate([mask] * 8, axis=0)
                    parts.append(
                        jnp.where(mask, scores[t][:, n * 128 : (n + 1) * 128], MASKED)
                    )
                best = functools.reduce(jnp.maximum, parts)
                span = slice(t * 1024 - origin, (t + 1) * 1024 - origin)
                top_old = top_ref[span, :]
                top = jnp.maximum(top_old, jnp.max(best, axis=1, keepdims=True))
                factor = jnp.exp2((top_old - top) * SCALE2)
                weights = [jnp.exp2((part - top) * SCALE2) for part in parts]
                sum_ref[span, :] = sum_ref[span, :] * factor + functools.reduce(jnp.add, weights)
                rounded = jnp.concatenate([w.astype(jnp.bfloat16) for w in weights], axis=1)
                mix_ref[span, :] = mix_ref[span, :] * factor + jnp.dot(
                    rounded, v, preferred_element_type=jnp.float32
                )
                top_ref[span, :] = top

    if last:
        for j in range(8):
            span = slice(j * 128, (j + 1) * 128)
            total = jnp.sum(sum_ref[span, :], axis=1, keepdims=True)
            out_ref[0:128, j * HD : (j + 1) * HD] = (mix_ref[span, :] / total).astype(jnp.bfloat16)
        total = got(key_refs[0], rider) + got(key_refs[1], rider) + energy_ref[...]
        put_wide(out_ref, total)
        out_ref[128:BLOCK, 512:1024] = jnp.zeros((16, 512), jnp.bfloat16)


def finish_kernel(first_ref, second_ref, attention_ref, captured_ref, share_ref):
    odd = place()[2]
    for swap in range(2):

        @pl.when(odd == swap)
        def _(swap=swap):
            for t, ref in enumerate((first_ref, second_ref)):
                head = t ^ swap
                attention_ref[:, head * 1024 : (head + 1) * 1024] = ref[0:128, :]

    received = [got_wide(first_ref), got_wide(second_ref)]
    row = lax.broadcasted_iota(jnp.int32, (RIDER, 128), 0)
    lane = lax.broadcasted_iota(jnp.int32, (RIDER, 128), 1)
    rows = lax.broadcasted_iota(jnp.int32, (2, 2), 0)
    columns = lax.broadcasted_iota(jnp.int32, (2, 2), 1)
    own, everything = {}, [0.0, 0.0]
    for g in range(2):
        sums = jnp.where(odd == g, received[0], received[1])
        for kind in range(2):
            n = 2 * g + kind
            captured_ref[n] = sums[:, n * RANK : (n + 1) * RANK] * (1.0 / TOKENS)
            here = lane == 64 * (1 - g)
            own[n] = jnp.sum(jnp.where(here & (row == kind), sums, 0.0))
            everything[kind] += 0.5 * jnp.sum(jnp.where(here & (row == kind + 2), sums, 0.0))
    share = jnp.zeros((2, 2), jnp.float32)
    for g in range(2):
        for kind in range(2):
            value = jnp.full((2, 2), KVH * own[2 * g + kind], jnp.float32) / everything[kind]
            share = jnp.where((rows == g) & (columns == kind), value, share)
    share_ref[...] = share


def vmem():
    return pl.BlockSpec(memory_space=pltpu.VMEM)


def rows(count):
    return jax.ShapeDtypeStruct((count, 256), jnp.bfloat16)


def small(kernel, out_shape, *inputs):
    return pl.pallas_call(
        kernel,
        out_shape=out_shape,
        in_specs=[vmem()] * len(inputs),
        out_specs=[vmem()] * len(out_shape),
        compiler_params=pltpu.CompilerParams(vmem_limit_bytes=6 * 1024 * 1024),
        cost_estimate=pl.CostEstimate(flops=1 << 20, bytes_accessed=1 << 18, transcendentals=0),
    )(*inputs)


def attend(q, arrays, units, state, tile=None, rider=None, energy=None):
    first, last = state is None, tile is not None
    wide = (2048, 128)
    carry = [
        jax.ShapeDtypeStruct(wide, jnp.bfloat16),
        jax.ShapeDtypeStruct((32, 128), jnp.float32),
        jax.ShapeDtypeStruct(wide, jnp.float32),
        jax.ShapeDtypeStruct(wide, jnp.float32),
        jax.ShapeDtypeStruct(wide, jnp.float32),
    ]
    tiles = (tile,) if last else (0, 1)
    keys = sum(128 * len(piece[4]) for unit in units for piece in unit)
    work = len(tiles) * 1024 * keys
    inputs = (list(q) if first else []) + list(arrays)
    aliases = {}
    if not first:
        if not last:
            aliases = {len(inputs) + n: n for n in range(5)}
        inputs += list(state)
    if last:
        inputs.append(energy)
        out_shape = [jax.ShapeDtypeStruct((BLOCK, 1024), jnp.bfloat16)]
        scratch = [pltpu.VMEM((1024, 128), jnp.float32)] * 3
    else:
        out_shape, scratch = carry, []
    return list(
        pl.pallas_call(
            functools.partial(attend_kernel, len(arrays), units, tiles, first, last, rider),
            out_shape=out_shape,
            in_specs=[vmem()] * len(inputs),
            out_specs=[vmem()] * len(out_shape),
            scratch_shapes=scratch,
            input_output_aliases=aliases,
            compiler_params=pltpu.CompilerParams(vmem_limit_bytes=20 * 1024 * 1024),
            cost_estimate=pl.CostEstimate(
                flops=4 * work * HD, bytes_accessed=1 << 20, transcendentals=work
            ),
            name="attend_last" if last else "attend",
        )(*inputs)
    )


def body(queries, keys, values, segments, basis):
    odd = lax.axis_index("y") & 1
    send0, send1, latents, energy = pl.pallas_call(
        prepare_kernel,
        out_shape=[
            rows(BLOCK + RIDER),
            rows(BLOCK + RIDER),
            jax.ShapeDtypeStruct((128, 128), jnp.bfloat16),
            jax.ShapeDtypeStruct((8, 128), jnp.float32),
        ],
        in_specs=[pl.BlockSpec(memory_space=pltpu.HBM)] * 4,
        out_specs=[vmem()] * 4,
        scratch_shapes=[
            pltpu.VMEM((128, 256), jnp.bfloat16),
            pltpu.VMEM((128, 256), jnp.bfloat16),
            pltpu.VMEM((1, 128), jnp.int32),
            pltpu.VMEM((2, 2, RANK, HD), jnp.bfloat16),
            pltpu.SemaphoreType.DMA((4,)),
        ],
        compiler_params=pltpu.CompilerParams(vmem_limit_bytes=66100000),
        name="prepare",
    )(keys, values, segments.reshape(1, 128), jnp.swapaxes(basis, 2, 3))
    kv = []
    for t, array in enumerate((send0, send1)):
        kv.append(lax.ppermute(array, COLUMN, to_heads(t)))
    slices = [lax.dynamic_slice_in_dim(queries, (odd ^ t) * 1024, 1024, 1) for t in range(2)]
    q = []
    for t in range(2):
        q.append(lax.ppermute(slices[t], COLUMN, to_heads(t)))
    energy = added(energy, "c", 1)
    energy = added(energy, "xl", 1)

    def partner(array):
        return lax.ppermute(array, "c", [(0, 1), (1, 0)])

    def after(state, *arrays):
        state[2], *arrays = lax.optimization_barrier((state[2], *arrays))
        return arrays

    def piece(array, row, distance, other):
        return (array, row, distance, other, (None,) if distance == 9 else (0, 1))

    message = rows(HALF + RIDER)
    (own,) = small(start_kernel, [message], *kv, energy)
    eight, one = shifted(own, 8), shifted(own, 1)
    twelve = shifted(own[HALF:], -4)
    up, down, both = small(
        once_kernel, [rows(HALF + RIDER + BLOCK), message, rows(3 * HALF)], own, eight, one
    )
    two, seven = shifted(up, 1), shifted(down, -1)
    other_first = partner(both)
    near, up = lax.optimization_barrier((own, up))
    state = attend(q, [near, eight], ((piece(0, 0, 0, False), piece(1, 0, 8, False)),), None)
    state = attend(
        None,
        [one, other_first],
        (
            (piece(0, 0, 1, False), piece(1, 2 * HALF, 1, True)),
            (piece(1, 0, 0, True), piece(1, HALF, 8, True)),
        ),
        state,
    )

    two, seven = after(state, two, seven)
    onward, both = small(split_kernel, [message, rows(2 * HALF + BLOCK)], two, seven)
    three, six = shifted(onward, 1), shifted(seven, -1)
    other_two_seven = partner(both)
    state = attend(None, [two, seven], ((piece(0, 0, 2, False), piece(1, 0, 7, False)),), state)
    state = attend(
        None, [other_two_seven], ((piece(0, 0, 2, True), piece(0, HALF, 7, True)),), state
    )

    three, six = after(state, three, six)
    four, five = shifted(three, 1), shifted(six, -1)
    (both,) = small(pair_kernel, [rows(2 * HALF)], three, six)
    other_three_six = partner(both)
    state = attend(None, [three, six], ((piece(0, 0, 3, False), piece(1, 0, 6, False)),), state)

    four, five = after(state, four, five)
    last, energy = small(
        total_kernel,
        [rows(2 * HALF + RIDER), jax.ShapeDtypeStruct((RIDER, 128), jnp.float32)],
        four,
        five,
        own,
        eight,
        one,
        two,
        three,
        seven,
        six,
        twelve,
    )
    other_last = partner(last)
    energy = lax.ppermute(energy, "y", [(i, i ^ 2) for i in range(4)])
    state = attend(
        None, [other_three_six], ((piece(0, 0, 3, True), piece(0, HALF, 6, True)),), state
    )
    units = (
        (piece(1, 0, 4, False), piece(1, HALF + RIDER, 5, False)),
        (piece(2, HALF + RIDER, 9, False), piece(3, 2 * HALF, 9, True)),
        (piece(0, 0, 4, True), piece(0, HALF + RIDER, 5, True)),
    )
    arrays = [other_last, last, two, other_two_seven]
    back = []
    for t in range(2):
        (mixed,) = attend(
            None, arrays, units, state, t, HALF, energy
        )
        back.append(lax.ppermute(mixed, COLUMN, [(d, s) for s, d in to_heads(t)]))
    attention, captured, share = small(
        finish_kernel,
        [
            jax.ShapeDtypeStruct((128, 2048), jnp.bfloat16),
            jax.ShapeDtypeStruct((4, RANK, RANK), jnp.float32),
            jax.ShapeDtypeStruct((2, 2), jnp.float32),
        ],
        *back,
    )
    return (attention, latents, captured.reshape(2, 2, RANK, RANK), share)


def solution(mesh):
    torus = Mesh(mesh.devices.reshape(2, 8, 4, 2, 2), ("a", "z", "y", "xl", "c"))
    in_specs = (P(SEQ, KV), P(SEQ, KV), P(SEQ, KV), P(SEQ), P(KV, None, None, None))
    out_specs = (P(SEQ, KV), P(SEQ, KV), P(KV, None, None, None), P(KV, None))

    return jax.shard_map(body, mesh=torus, in_specs=in_specs, out_specs=out_specs, check_vma=False)
```
